32 devices in a mesh: leaf: 4 (over z), row: 2 (over x), col: 4 (over y, core).
Axes of the slice: x: 2, y: 2, z: 4, core: 2. Of those that a mesh axis runs over, the one named last changes fastest.
Arguments:
- pivot: float32 [4, 1024, 1024], P('leaf', 'row', 'col'), as said below
- border: float32 [4, 3072, 1024], P('leaf', 'row', 'col'), may hold values from -0.065625 to 0.065625
- update: float32 [4, 3072, 3072], P('leaf', 'row', 'col'), as said below
- child_map: int32 [4, 3072], replicated, may hold values from 0 to 4607, as said below
- parent_diag: float32 [4, 2304], P('leaf', 'row'), may hold values from 0.5 to 4
Outputs:
- factor_pivot: float32 [4, 1024, 1024], P('leaf', 'row', 'col')
- factor_border: float32 [4, 3072, 1024], P('leaf', 'row', 'col')
- parent_front: float32 [4, 2304, 4608], P('leaf', 'row', 'col')
The draws below stay inside these ranges and needn't reach their ends.
Inputs may be any that keep to these rules, and one draw needn't show every extreme that they name: Each row child_map[l] is increasing with distinct entries, and its i-th block of 768 entries lies among parent rows i * 1152 to (i+1) * 1152 - 1. Each pivot[l] is symmetric positive definite. Each update[l] is symmetric.
All inputs are finite; a program needn't handle non-finite values.
Results may differ from the reference program's by a relative error of at most 0.00007.
Values sent between devices are 32-bit elements; how exact they have to be, the bound alone decides.
A program may use at most 128 MiB of HBM per device.

```python
import math
import jax
import jax.numpy as jnp
from jax import lax

PANEL = 1024
UPD = 3072
PARENT = 4608
CHILD = 4096
LEAVES = 4
NB = 4
RB = 1152
N_ROW = 2


def symmetric_part(key, count, order):
    noise = jax.random.normal(key, (count, order, order), jnp.float32)
    return (noise + jnp.swapaxes(noise, 1, 2)) * (0.7 / math.sqrt(2.0 * CHILD))


def dominant(key, order):
    first, second = jax.random.split(key)
    diagonal = jax.random.uniform(second, (LEAVES, order), jnp.float32, 2.0, 4.0)
    return symmetric_part(first, LEAVES, order) + diagonal[:, :, None] * jnp.eye(order, dtype=jnp.float32)[None]


def coupling(key, order):
    places = jnp.arange(order, dtype=jnp.float32)
    distance = jnp.abs(places[:, None] - places[None, :])
    kernel = (3.0 + 6.0 * jnp.exp(-distance * (4.0 / order))) / order
    strength = jax.random.uniform(key, (LEAVES,), jnp.float32, 0.8, 1.6)
    return strength[:, None, None] * kernel[None]


def draw_pivot(key, part):
    base = dominant(jax.random.fold_in(key, 11), PANEL)
    return base + coupling(jax.random.fold_in(key, 19), PANEL)


def draw_update(key, part):
    return dominant(jax.random.fold_in(key, 13), UPD)


def draw_child_map(key, part):
    keys = jax.random.split(jax.random.fold_in(key, 17), LEAVES * NB)

    def choose(single):
        return jnp.sort(jax.random.permutation(single, PARENT // NB)[:UPD // NB])
    picked = jax.vmap(choose)(keys).reshape(LEAVES, NB, UPD // NB)
    offsets = (jnp.arange(NB, dtype=jnp.int32) * (PARENT // NB))[None, :, None]
    return (picked.astype(jnp.int32) + offsets).reshape(LEAVES, UPD).astype(jnp.int32)


def block_scale(key, extent, cuts, least, largest):
    gain = 1.0
    for dim, blocks in cuts:
        heights = jax.random.uniform(jax.random.fold_in(jax.random.fold_in(key, 6), dim), (blocks,), jnp.float32, least / len(cuts), largest / len(cuts))
        gain = gain * jnp.repeat(jnp.exp(heights), extent[dim] // blocks).reshape((-1,) + (1,) * (len(extent) - 1 - dim))
    return gain


def bell_draw(key, shape, spread, bound, cuts=(), held_as=jnp.bfloat16):
    array = jax.random.normal(key, shape, jnp.float32) * spread
    if len(cuts) > 0:
        array = block_scale(key, shape, cuts, -0.22, 0.18) * array
    return jnp.clip(array, min=-bound, max=bound).astype(held_as)


def setup_inputs(seed: int = 0) -> dict:
    splits = jax.random.split(jax.random.key(seed), 6)
    return {
        "pivot": draw_pivot(jax.random.fold_in(splits[5], 71), 0),
        "border": bell_draw(splits[1], (LEAVES, UPD, PANEL), (0.7 / (CHILD ** 0.5)), 0.065625, ((0, 4), (1, 2), (2, 4)), jnp.float32),
        "update": draw_update(jax.random.fold_in(splits[5], 71), 0),
        "child_map": draw_child_map(jax.random.fold_in(splits[5], 71), 0),
        "parent_diag": jnp.clip(jnp.exp(math.log(4.0) - 2.0794415 * jax.random.uniform(splits[4], (LEAVES, PARENT // 2), jnp.float32) ** block_scale(splits[4], (LEAVES, PARENT // 2), ((0, 4), (1, 2)), -0.2, 0.2)), 0.5, 4.0),
    }


def eliminate(blocks):
    piv, bord, upd = blocks
    lower = jnp.linalg.cholesky(piv)
    below = lax.linalg.triangular_solve(lower, bord, left_side=False, lower=True, transpose_a=True)
    schur = upd - jnp.dot(below.astype(jnp.float32), below.T.astype(jnp.float32), precision=lax.Precision.HIGHEST, preferred_element_type=jnp.float32)
    return (lower, below, schur)

def reference(pivot, border, update, child_map, parent_diag):
    lowers, belows, schurs = lax.map(eliminate, (pivot, border, update))
    fronts = []
    for pair in range(LEAVES // 2):
        front = jnp.zeros((PARENT, PARENT), jnp.float32)
        for side in range(2):
            index = child_map[2 * pair + side]
            front = front.at[index[:, None], index[None, :]].add(schurs[2 * pair + side])
        diag_rows = parent_diag[2 * pair:2 * pair + 2].reshape(2, N_ROW, RB).transpose(1, 0, 2).reshape(PARENT)
        front = front + jnp.diag(diag_rows)
        fronts.append(front.reshape(N_ROW, 2, RB, PARENT).transpose(1, 0, 2, 3).reshape(2, PARENT // 2, PARENT))
    return (lowers, belows, jnp.concatenate(fronts, axis=0))
```

```python
import jax
import jax.numpy as jnp
from jax import lax
from jax.experimental import pallas as pl
from jax.experimental.pallas import tpu as pltpu
from jax.sharding import PartitionSpec as P

BLOCK = 128
CHUNKS = 2
PANEL = 8
HIGH = lax.Precision.HIGH


def exact_dot(left, right):
    return jnp.dot(left, right, precision=lax.Precision.HIGHEST, preferred_element_type=jnp.float32)


def factor_small(entry):
    work = {key: value for key, value in entry.items()}
    lower = {}
    inverse = {}
    for k in range(PANEL):
        scale = lax.rsqrt(work[k, k])
        for i in range(k + 1, PANEL):
            lower[i, k] = work[i, k] * scale
        for j in range(k + 1, PANEL):
            for i in range(j, PANEL):
                work[i, j] = work[i, j] - lower[i, k] * lower[j, k]
        inverse[k, k] = scale
        for j in range(k):
            total = lower[k, j] * inverse[j, j]
            for m in range(j + 1, k):
                total = total + lower[k, m] * inverse[m, j]
            inverse[k, j] = -(total * scale)
    return inverse


def factor_block(diag, upper, inv):
    lane8 = lax.broadcasted_iota(jnp.int32, (PANEL, BLOCK), 1)
    lane_all = lax.broadcasted_iota(jnp.int32, (BLOCK, BLOCK), 1)

    def panel_step(p, carry):
        base = p * PANEL
        start = pl.multiple_of(base, PANEL)
        rows = diag[pl.ds(start, PANEL), :]
        full = diag[...]
        entry = {}
        for b in range(PANEL):
            index = jnp.zeros((PANEL, BLOCK), jnp.int32) + (base + b)
            col = jnp.take_along_axis(rows, index, axis=1, mode="promise_in_bounds")
            for a in range(b, PANEL):
                entry[a, b] = jnp.broadcast_to(col[a : a + 1, :], (PANEL, BLOCK))
        inverse = factor_small(entry)
        inside = (lane8 >= base) & (lane8 < base + PANEL)
        plain = []
        augmented = []
        for k in range(PANEL):
            row = jnp.broadcast_to(rows[k : k + 1, :], (PANEL, BLOCK))
            plain.append(row)
            augmented.append(jnp.where(inside, (lane8 == base + k).astype(jnp.float32), row))
        solved = []
        for a in range(PANEL):
            up = inverse[a, 0] * plain[0]
            au = inverse[a, 0] * augmented[0]
            for k in range(1, a + 1):
                up = up + inverse[a, k] * plain[k]
                au = au + inverse[a, k] * augmented[k]
            solved.append(au)
            keep = lane8 >= base + a
            upper[pl.ds(start + a, 1), :] = jnp.where(keep, up, 0.0)[0:1, :]
            inv[pl.ds(start + a, 1), :] = jnp.where(lane8 <= base + a, au, 0.0)[0:1, :]
        inside_all = (lane_all >= base) & (lane_all < base + PANEL)
        trailing = jnp.where(inside_all, 0.0, full)
        for m in range(PANEL):
            gain = inverse[m, m] * solved[m]
            for a in range(m + 1, PANEL):
                gain = gain + inverse[a, m] * solved[a]
            index = jnp.zeros((BLOCK, BLOCK), jnp.int32) + (base + m)
            col = jnp.take_along_axis(full, index, axis=1, mode="promise_in_bounds")
            trailing = trailing - col * jnp.broadcast_to(gain[0:1, :], (BLOCK, BLOCK))
        diag[...] = trailing
        return carry

    lax.fori_loop(0, BLOCK // PANEL, panel_step, 0)


def split_three(value):
    top = value.astype(jnp.bfloat16)
    rest = value - top.astype(jnp.float32)
    mid = rest.astype(jnp.bfloat16)
    return top, mid, (rest - mid.astype(jnp.float32)).astype(jnp.bfloat16)


def factor_kernel(pivot, upper_out, inverse_out, work, diag, upper, inv, panel, parts):
    factor_core(pivot, upper_out, inverse_out, work, diag, upper, inv, panel, parts, None)


def factor_core(pivot, upper_out, inverse_out, work, diag, upper, inv, panel, parts, pump):
    order = work.shape[0]
    count = order // BLOCK
    lane = lax.broadcasted_iota(jnp.int32, (BLOCK, order), 1)
    pieces, piece_rows, piece_cols = pivot.shape
    across = order // piece_cols
    for index in range(pieces):
        first_row = index // across * piece_rows
        first_col = index % across * piece_cols
        if first_row < first_col + piece_cols:
            work[pl.ds(first_row, piece_rows), pl.ds(first_col, piece_cols)] = pivot[index]
        else:
            work[pl.ds(first_row, piece_rows), pl.ds(first_col, piece_cols)] = jnp.zeros(
                (piece_rows, piece_cols), jnp.float32
            )

    def block_step(kb, carry):
        if pump is not None:
            pump(kb)
        start = pl.multiple_of(kb * BLOCK, BLOCK)
        here = pl.ds(start, BLOCK)
        diag[...] = work[here, here]
        factor_block(diag, upper, inv)
        work[here, here] = jnp.where(
            lax.broadcasted_iota(jnp.int32, (BLOCK, BLOCK), 0)
            == lax.broadcasted_iota(jnp.int32, (BLOCK, BLOCK), 1),
            1.0,
            0.0,
        )
        panel[...] = exact_dot(inv[...], work[here, :])
        solved = panel[...]
        inverse_out[here, :] = jnp.where(lane < start + BLOCK, solved, 0.0)
        upper_out[here, :] = jnp.where(lane >= start + BLOCK, solved, 0.0)
        upper_out[here, here] = upper[...]

        top, mid, low = split_three(solved)
        parts[0, :BLOCK, :] = top
        parts[0, BLOCK:, :] = top
        parts[1, :BLOCK, :] = mid
        parts[1, BLOCK:, :] = mid
        parts[2, :BLOCK, :] = low
        parts[2, BLOCK:, :] = top

        def row_step(ib, carry):
            there = pl.ds(pl.multiple_of(ib * BLOCK, BLOCK), BLOCK)
            top, mid, low = split_three(panel[:, there].T)
            both = jnp.concatenate([top, mid], axis=1)
            ends = jnp.concatenate([top, low], axis=1)
            change = jnp.dot(ends, parts[2], preferred_element_type=jnp.float32)
            change = change + jnp.dot(both, parts[1], preferred_element_type=jnp.float32)
            change = change + jnp.dot(both, parts[0], preferred_element_type=jnp.float32)
            work[there, here] = jnp.zeros((BLOCK, BLOCK), jnp.float32)
            work[there, :] = work[there, :] - change
            return carry

        lax.fori_loop(kb + 1, count, row_step, 0)
        return carry

    lax.fori_loop(0, count, block_step, 0)


def factor(pivot, order):
    spec = pl.BlockSpec(memory_space=pltpu.VMEM)
    shape = jax.ShapeDtypeStruct((order, order), jnp.float32)
    return pl.pallas_call(
        factor_kernel,
        out_shape=(shape, shape),
        in_specs=[spec],
        out_specs=(spec, spec),
        scratch_shapes=[
            pltpu.VMEM((order, order), jnp.float32),
            pltpu.VMEM((BLOCK, BLOCK), jnp.float32),
            pltpu.VMEM((BLOCK, BLOCK), jnp.float32),
            pltpu.VMEM((BLOCK, BLOCK), jnp.float32),
            pltpu.VMEM((BLOCK, order), jnp.float32),
            pltpu.VMEM((3, 2 * BLOCK, order), jnp.bfloat16),
        ],
        compiler_params=pltpu.CompilerParams(vmem_limit_bytes=40 * 2**20),
        cost_estimate=pl.CostEstimate(
            flops=60 * order**3, bytes_accessed=12 * order * order, transcendentals=order
        ),
        name="factor",
    )(pivot)


def flip(value):
    return value + 1 - 2 * (value % 2)


def grid_plan():
    leaf = lax.axis_index("leaf")
    row = lax.axis_index("row")
    col = lax.axis_index("col")
    core = col % 2
    cross = (col + 2) % 4
    mate = flip(col)
    return {
        "row": row,
        "col": col,
        "core": core,
        "half": col // 2,
        "mate": (leaf, row, mate),
        "side": (leaf, row, cross),
        "over": (leaf, 1 - row, col),
        "far": (leaf, 1 - row, cross),
    }


def remote(src, dst, send, recv, target):
    return pltpu.make_async_remote_copy(
        src_ref=src,
        dst_ref=dst,
        send_sem=send,
        recv_sem=recv,
        device_id=target,
        device_id_type=pl.DeviceIdType.MESH,
    )


def piece_needed(row, col, chunk):
    return col >= 2 * row + chunk


def gather_factor_kernel(
    pivot, border, pivot_out, inverse_out, rows_out, cols_out,
    stack, relay, work, upper_all, diag, upper, inv, panel, parts,
    local_sem, psend, precv, fsend, frecv, bsend, brecv, xsend, xrecv,
):
    plan = grid_plan()
    row, col, core, half = plan["row"], plan["col"], plan["core"], plan["half"]
    piece_rows, piece_cols = pivot.shape
    rows_local = border.shape[0]
    block = rows_local // 2
    step = piece_rows // 2
    barrier = pltpu.get_barrier_semaphore()
    for name in ("mate", "side", "over", "far"):
        pl.semaphore_signal(
            barrier, inc=1, device_id=plan[name], device_id_type=pl.DeviceIdType.MESH
        )
    mine = row * 4 + col
    keep_pivot = pltpu.make_async_copy(pivot, stack.at[mine], local_sem.at[0])
    keep_pivot.start()

    def slot_cols(which):
        return pl.ds(pl.multiple_of(which * piece_cols, piece_cols), piece_cols)

    def slot_rows(which):
        return pl.ds(pl.multiple_of(which * block, block), block)

    keep_border = pltpu.make_async_copy(border, rows_out.at[:, slot_cols(col)], local_sem.at[1])
    keep_border.start()
    pl.semaphore_wait(barrier, 4)

    def own_piece(index, name, chunk):
        there = pl.ds(chunk * step, step)
        return remote(
            pivot.at[there], stack.at[mine, there],
            psend.at[index, chunk], precv.at[index, chunk], plan[name],
        )

    def pass_piece(index, chunk, source_row, source_col):
        there = pl.ds(chunk * step, step)
        place = source_row * 4 + source_col
        return remote(
            stack.at[place, there], stack.at[place, there],
            fsend.at[index, chunk], frecv.at[index, chunk], plan["mate"],
        )

    names = ("over", "side", "far", "mate")
    for chunk in range(2):
        @pl.when(piece_needed(row, col, chunk))
        def _(chunk=chunk):
            for index, name in enumerate(names):
                own_piece(index, name, chunk).start()

    def to_side(part):
        there = slot_rows(part)
        return remote(
            border.at[there], rows_out.at[there, slot_cols(col)],
            bsend.at[0, part], brecv.at[0, part], plan["side"],
        )

    def to_mate(part):
        there = slot_rows(part)
        return remote(
            border.at[there], rows_out.at[there, slot_cols(col)],
            bsend.at[1, part], brecv.at[1, part], plan["mate"],
        )

    cross = (col + 2) % 4
    mate = flip(col)
    mate_cross = (mate + 2) % 4

    def pass_side(part):
        there = slot_rows(part)
        return remote(
            rows_out.at[there, slot_cols(cross)], rows_out.at[there, slot_cols(cross)],
            bsend.at[2, part], brecv.at[2, part], plan["mate"],
        )

    def to_relay():
        return remote(border.at[slot_rows(core)], relay, xsend.at[0], xrecv.at[0], plan["over"])

    def from_relay():
        return remote(relay, cols_out.at[:, slot_cols(col)], xsend.at[1], xrecv.at[1], plan["side"])

    def over_cols(index, source, which):
        return remote(
            source, cols_out.at[:, slot_cols(which)],
            xsend.at[2 + index], xrecv.at[2 + index], plan["over"],
        )

    for part in range(2):
        to_side(part).start()
        to_mate(part).start()

    on_diag = row == half

    @pl.when(on_diag)
    def _():
        over_cols(0, border.at[slot_rows(core)], col).start()

    @pl.when(row != half)
    def _():
        to_relay().start()

    for chunk in range(2):
        for index, (source_row, source_col) in enumerate(
            ((1 - row, col), (row, cross), (1 - row, cross))
        ):
            @pl.when(piece_needed(source_row, source_col, chunk))
            def _(index=index, chunk=chunk, source_row=source_row, source_col=source_col):
                own_piece(index, names[index], chunk).wait_recv()
                pass_piece(index, chunk, source_row, source_col).start()

    for chunk in range(2):
        @pl.when(piece_needed(row, mate, chunk))
        def _(chunk=chunk):
            own_piece(3, "mate", chunk).wait_recv()
        for index, (source_row, source_col) in enumerate(
            ((1 - row, mate), (row, mate_cross), (1 - row, mate_cross))
        ):
            @pl.when(piece_needed(source_row, source_col, chunk))
            def _(index=index, chunk=chunk):
                pass_piece(index, chunk, 0, 0).wait_recv()
    keep_pivot.wait()

    def pump(kb):
        @pl.when(kb == 1)
        def _():
            keep_border.wait()
            for part in range(2):
                to_mate(part).wait_recv()

            @pl.when(on_diag)
            def _():
                over_cols(
                    1, rows_out.at[slot_rows(core), slot_cols(mate)], mate
                ).start()

        @pl.when(kb == 4)
        def _():
            @pl.when(on_diag)
            def _():
                to_relay().wait_recv()
                from_relay().start()

        for part in range(2):
            @pl.when(kb == 3 + 2 * part)
            def _(part=part):
                to_side(part).wait_recv()
                pass_side(part).start()

        @pl.when(kb == 6)
        def _():
            for part in range(2):
                pass_side(part).wait_recv()

            @pl.when(on_diag)
            def _():
                over_cols(
                    2, rows_out.at[slot_rows(core), slot_cols(mate_cross)], mate_cross
                ).start()

    factor_core(stack, upper_all, inverse_out, work, diag, upper, inv, panel, parts, pump)
    piece = upper_all[
        pl.ds(pl.multiple_of(col * piece_cols, piece_cols), piece_cols),
        pl.ds(pl.multiple_of(row * piece_rows, piece_rows), piece_rows),
    ]
    pivot_out[...] = piece.T

    @pl.when(row != half)
    def _():
        to_relay().wait_send()
        from_relay().wait_recv()
        for index in range(3):
            over_cols(index, border.at[slot_rows(core)], col).wait_recv()

    @pl.when(on_diag)
    def _():
        from_relay().wait_send()
        for index in range(3):
            over_cols(index, border.at[slot_rows(core)], col).wait_send()

    for part in range(2):
        to_side(part).wait_send()
        to_mate(part).wait_send()
        pass_side(part).wait_send()
    for chunk in range(2):
        @pl.when(piece_needed(row, col, chunk))
        def _(chunk=chunk):
            for index, name in enumerate(names):
                own_piece(index, name, chunk).wait_send()
        for index, (source_row, source_col) in enumerate(
            ((1 - row, col), (row, cross), (1 - row, cross))
        ):
            @pl.when(piece_needed(source_row, source_col, chunk))
            def _(index=index, chunk=chunk):
                pass_piece(index, chunk, 0, 0).wait_send()


def gather_factor(pivot, border, order):
    piece_rows, piece_cols = pivot.shape
    rows_local = border.shape[0]
    block = rows_local // 2
    vmem = pl.BlockSpec(memory_space=pltpu.VMEM)
    anywhere = pl.BlockSpec(memory_space=pl.ANY)
    dma = pltpu.SemaphoreType.DMA
    return pl.pallas_call(
        gather_factor_kernel,
        out_shape=(
            jax.ShapeDtypeStruct((piece_rows, piece_cols), jnp.float32),
            jax.ShapeDtypeStruct((order, order), jnp.float32),
            jax.ShapeDtypeStruct((rows_local, order), jnp.float32),
            jax.ShapeDtypeStruct((block, order), jnp.float32),
        ),
        in_specs=[anywhere, anywhere],
        out_specs=(vmem, vmem, anywhere, anywhere),
        scratch_shapes=[
            pltpu.VMEM((8, piece_rows, piece_cols), jnp.float32),
            pltpu.VMEM((block, piece_cols), jnp.float32),
            pltpu.VMEM((order, order), jnp.float32),
            pltpu.VMEM((order, order), jnp.float32),
            pltpu.VMEM((BLOCK, BLOCK), jnp.float32),
            pltpu.VMEM((BLOCK, BLOCK), jnp.float32),
            pltpu.VMEM((BLOCK, BLOCK), jnp.float32),
            pltpu.VMEM((BLOCK, order), jnp.float32),
            pltpu.VMEM((3, 2 * BLOCK, order), jnp.bfloat16),
            dma((2,)), dma((4, 2)), dma((4, 2)), dma((3, 2)), dma((3, 2)),
            dma((3, 2)), dma((3, 2)), dma((5,)), dma((5,)),
        ],
        compiler_params=pltpu.CompilerParams(
            vmem_limit_bytes=48 * 2**20, collective_id=0, has_side_effects=True
        ),
        cost_estimate=pl.CostEstimate(
            flops=60 * order**3, bytes_accessed=12 * order * order, transcendentals=order
        ),
        name="gather_factor",
    )(pivot, border)


def high_dot_t(left, right):
    return lax.dot_general(
        left, right, (((1,), (1,)), ((), ())), precision=HIGH, preferred_element_type=jnp.float32
    )


def split_two(value):
    top = lax.reduce_precision(value, 8, 7)
    return top.astype(jnp.bfloat16), (value - top).astype(jnp.bfloat16)


def one_hot(targets, size):
    return (jnp.arange(size, dtype=jnp.int32)[:, None] == targets[None, :]).astype(jnp.bfloat16)


def pick_dot(left, right, dims):
    return lax.dot_general(left, right, (dims, ((), ())), preferred_element_type=jnp.float32)


def place_blocks(blocks, rows_to, cols_to, out_rows, out_cols):
    col_hot = one_hot(cols_to, out_cols)
    first = 0
    placed = None
    for block in blocks:
        count = block.shape[0]
        row_hot = one_hot(rows_to[first : first + count], out_rows)
        first += count
        top, rest = split_two(block)
        wide = pick_dot(top, col_hot, ((1,), (1,))) + pick_dot(rest, col_hot, ((1,), (1,)))
        top, rest = split_two(wide)
        part = pick_dot(row_hot, top, ((1,), (0,))) + pick_dot(row_hot, rest, ((1,), (0,)))
        placed = part if placed is None else placed + part
    return placed


def column_border(bord, full_rows, nrow, ncol, cols_local, row_index, col_index):
    rows_local, width = bord.shape
    if nrow == 2 and rows_local % cols_local == 0:
        per_row = rows_local // cols_local
        mine = lax.dynamic_slice_in_dim(full_rows, (col_index % per_row) * cols_local, cols_local, 0)
        received = jnp.zeros((cols_local, full_rows.shape[1]), bord.dtype)
        for shift in range(ncol):
            pairs = []
            for c in range(ncol):
                home = c // per_row
                pairs.append((home * ncol + (c + shift) % ncol, (1 - home) * ncol + c))
            target = (col_index - shift + ncol) % ncol
            part = lax.dynamic_slice_in_dim(bord, (target % per_row) * cols_local, cols_local, 0)
            moved = lax.ppermute(part, ("row", "col"), pairs)
            place = (col_index + shift) % ncol * width
            received = lax.dynamic_update_slice_in_dim(received, moved, place, 1)
        return jnp.where(row_index == col_index // per_row, mine, received)
    whole = lax.all_gather(full_rows, "row", axis=0, tiled=True)
    return lax.dynamic_slice_in_dim(whole, col_index * cols_local, cols_local, 0)


def on_device(pivot, border, update, child_map, parent_diag):
    nrow = lax.axis_size("row")
    ncol = lax.axis_size("col")
    row_index = lax.axis_index("row")
    col_index = lax.axis_index("col")
    leaf_index = lax.axis_index("leaf")
    piece = pivot[0]
    piece_rows, piece_cols = piece.shape
    bord = border[0]
    rows_local = bord.shape[0]
    trailing = update[0]
    cols_local = trailing.shape[1]
    if nrow == 2 and ncol == 4 and piece_rows == 2 * piece_cols and rows_local == 2 * cols_local:
        pivot_out, inverse, full_rows, col_rows = gather_factor(piece, bord, nrow * piece_rows)
        near = lax.dynamic_slice_in_dim(full_rows, (col_index % 2) * cols_local, cols_local, 0)
        col_rows = jnp.where(row_index == col_index // 2, near, col_rows)
    else:
        stacked = lax.all_gather(piece[None], ("row", "col"), axis=0, tiled=True)
        stacked, bord = lax.optimization_barrier((stacked, bord))
        upper, inverse = factor(stacked, nrow * piece_rows)
        pivot_out = lax.dynamic_slice(
            upper, (col_index * piece_cols, row_index * piece_rows), (piece_cols, piece_rows)
        ).T
        full_rows = lax.all_gather(bord, "col", axis=1, tiled=True)
        col_rows = column_border(bord, full_rows, nrow, ncol, cols_local, row_index, col_index)
    factor_cols = high_dot_t(col_rows, inverse)

    half_rows = parent_diag.shape[1]
    block_rows = 2 * half_rows
    parent_cols = block_rows * nrow // ncol
    side = leaf_index % 2
    partner = leaf_index + 1 - 2 * side
    total_cols = child_map.shape[1]
    own_map = lax.dynamic_slice(child_map, (leaf_index, 0), (1, total_cols))[0]
    partner_map = lax.dynamic_slice(child_map, (partner, 0), (1, total_cols))[0]
    swap = [(source, source ^ 1) for source in range(lax.axis_size("leaf"))]

    map_block = total_cols // max(nrow, ncol)
    halves = rows_local % (2 * map_block) == 0
    if halves:
        kept = rows_local // 2
        own_start = side * kept
        sent_start = (1 - side) * kept

        def schur_rows(start, size):
            rows = lax.dynamic_slice_in_dim(full_rows, start, size, 0)
            below = high_dot_t(rows, inverse)
            part = lax.dynamic_slice_in_dim(trailing, start, size, 0)
            return below, part - high_dot_t(below, factor_cols)

        sent_parts = []
        sibling = []
        chunk = kept // CHUNKS
        for index in range(CHUNKS):
            below, sent = schur_rows(sent_start + index * chunk, chunk)
            sent_parts.append(below)
            sibling.append(lax.ppermute(sent, "leaf", swap))
        sent_below = jnp.concatenate(sent_parts, axis=0)
        own_below, own = schur_rows(own_start, kept)
        own_slice = lax.dynamic_slice_in_dim(own_below, col_index * piece_cols, piece_cols, 1)
        sent_slice = lax.dynamic_slice_in_dim(sent_below, col_index * piece_cols, piece_cols, 1)
        border_out = jnp.where(
            side == 0,
            jnp.concatenate([own_slice, sent_slice], axis=0),
            jnp.concatenate([sent_slice, own_slice], axis=0),
        )
    else:
        kept = rows_local
        own_start = 0
        factor_rows = high_dot_t(full_rows, inverse)
        own = trailing - high_dot_t(factor_rows, factor_cols)
        sibling = [lax.ppermute(own, "leaf", swap)]
        border_out = lax.dynamic_slice_in_dim(factor_rows, col_index * piece_cols, piece_cols, 1)

    def my_half(blocks, mapping):
        rows_to = (
            lax.dynamic_slice_in_dim(mapping, row_index * rows_local + own_start, kept)
            - row_index * block_rows
            - side * half_rows
        )
        cols_to = (
            lax.dynamic_slice_in_dim(mapping, col_index * cols_local, cols_local)
            - col_index * parent_cols
        )
        return place_blocks(blocks, rows_to, cols_to, half_rows, parent_cols)

    global_rows = row_index * block_rows + side * half_rows + jnp.arange(half_rows, dtype=jnp.int32)
    global_cols = col_index * parent_cols + jnp.arange(parent_cols, dtype=jnp.int32)
    diagonal = jnp.where(global_rows[:, None] == global_cols[None, :], parent_diag[0][:, None], 0.0)
    parent_out = my_half([own], own_map) + diagonal + my_half(sibling, partner_map)
    return (pivot_out[None], border_out[None], parent_out[None])


def solution(mesh):
    placed = (
        P("leaf", "row", "col"),
        P("leaf", "row", "col"),
        P("leaf", "row", "col"),
        P(),
        P("leaf", "row"),
    )
    return jax.shard_map(
        on_device,
        mesh=mesh,
        in_specs=placed,
        out_specs=(P("leaf", "row", "col"), P("leaf", "row", "col"), P("leaf", "row", "col")),
        check_vma=False,
    )
```

```python
import jax
import jax.numpy as jnp
from jax import lax
from jax.experimental import pallas as pl
from jax.experimental.pallas import tpu as pltpu
from jax.sharding import PartitionSpec as P

BLOCK = 128
CHUNKS = 2
PANEL = 8
HIGH = lax.Precision.HIGH


def exact_dot(left, right):
    return jnp.dot(left, right, precision=lax.Precision.HIGHEST, preferred_element_type=jnp.float32)


def factor_small(entry):
    work = {key: value for key, value in entry.items()}
    lower = {}
    inverse = {}
    for k in range(PANEL):
        scale = lax.rsqrt(work[k, k])
        for i in range(k + 1, PANEL):
            lower[i, k] = work[i, k] * scale
        for j in range(k + 1, PANEL):
            for i in range(j, PANEL):
                work[i, j] = work[i, j] - lower[i, k] * lower[j, k]
        inverse[k, k] = scale
        for j in range(k):
            total = lower[k, j] * inverse[j, j]
            for m in range(j + 1, k):
                total = total + lower[k, m] * inverse[m, j]
            inverse[k, j] = -(total * scale)
    return inverse


def factor_block(diag, upper, inv):
    lane8 = lax.broadcasted_iota(jnp.int32, (PANEL, BLOCK), 1)
    lane_all = lax.broadcasted_iota(jnp.int32, (BLOCK, BLOCK), 1)

    def panel_step(p, carry):
        base = p * PANEL
        start = pl.multiple_of(base, PANEL)
        rows = diag[pl.ds(start, PANEL), :]
        full = diag[...]
        entry = {}
        for b in range(PANEL):
            index = jnp.zeros((PANEL, BLOCK), jnp.int32) + (base + b)
            col = jnp.take_along_axis(rows, index, axis=1, mode="promise_in_bounds")
            for a in range(b, PANEL):
                entry[a, b] = jnp.broadcast_to(col[a : a + 1, :], (PANEL, BLOCK))
        inverse = factor_small(entry)
        inside = (lane8 >= base) & (lane8 < base + PANEL)
        plain = []
        augmented = []
        for k in range(PANEL):
            row = jnp.broadcast_to(rows[k : k + 1, :], (PANEL, BLOCK))
            plain.append(row)
            augmented.append(jnp.where(inside, (lane8 == base + k).astype(jnp.float32), row))
        solved = []
        for a in range(PANEL):
            up = inverse[a, 0] * plain[0]
            au = inverse[a, 0] * augmented[0]
            for k in range(1, a + 1):
                up = up + inverse[a, k] * plain[k]
                au = au + inverse[a, k] * augmented[k]
            solved.append(au)
            keep = lane8 >= base + a
            upper[pl.ds(start + a, 1), :] = jnp.where(keep, up, 0.0)[0:1, :]
            inv[pl.ds(start + a, 1), :] = jnp.where(lane8 <= base + a, au, 0.0)[0:1, :]
        inside_all = (lane_all >= base) & (lane_all < base + PANEL)
        trailing = jnp.where(inside_all, 0.0, full)
        for m in range(PANEL):
            gain = inverse[m, m] * solved[m]
            for a in range(m + 1, PANEL):
                gain = gain + inverse[a, m] * solved[a]
            index = jnp.zeros((BLOCK, BLOCK), jnp.int32) + (base + m)
            col = jnp.take_along_axis(full, index, axis=1, mode="promise_in_bounds")
            trailing = trailing - col * jnp.broadcast_to(gain[0:1, :], (BLOCK, BLOCK))
        diag[...] = trailing
        return carry

    lax.fori_loop(0, BLOCK // PANEL, panel_step, 0)


def split_three(value):
    top = value.astype(jnp.bfloat16)
    rest = value - top.astype(jnp.float32)
    mid = rest.astype(jnp.bfloat16)
    return top, mid, (rest - mid.astype(jnp.float32)).astype(jnp.bfloat16)


def factor_steps(work, diag, upper, inv, panel, parts, finish, pump=None):
    order = work.shape[0]
    count = order // BLOCK

    def block_step(kb, carry):
        if pump is not None:
            pump(kb)
        start = pl.multiple_of(kb * BLOCK, BLOCK)
        here = pl.ds(start, BLOCK)
        diag[...] = work[here, here]
        factor_block(diag, upper, inv)
        work[here, here] = jnp.where(
            lax.broadcasted_iota(jnp.int32, (BLOCK, BLOCK), 0)
            == lax.broadcasted_iota(jnp.int32, (BLOCK, BLOCK), 1),
            1.0,
            0.0,
        )
        panel[...] = exact_dot(inv[...], work[here, :])
        solved = panel[...]
        finish(start, here, solved)

        top, mid, low = split_three(solved)
        parts[0, :BLOCK, :] = top
        parts[0, BLOCK:, :] = top
        parts[1, :BLOCK, :] = mid
        parts[1, BLOCK:, :] = mid
        parts[2, :BLOCK, :] = low
        parts[2, BLOCK:, :] = top

        def row_step(ib, carry):
            there = pl.ds(pl.multiple_of(ib * BLOCK, BLOCK), BLOCK)
            top, mid, low = split_three(panel[:, there].T)
            both = jnp.concatenate([top, mid], axis=1)
            ends = jnp.concatenate([top, low], axis=1)
            change = jnp.dot(ends, parts[2], preferred_element_type=jnp.float32)
            change = change + jnp.dot(both, parts[1], preferred_element_type=jnp.float32)
            change = change + jnp.dot(both, parts[0], preferred_element_type=jnp.float32)
            work[there, here] = jnp.zeros((BLOCK, BLOCK), jnp.float32)
            work[there, :] = work[there, :] - change
            return carry

        lax.fori_loop(kb + 1, count, row_step, 0)
        return carry

    lax.fori_loop(0, count, block_step, 0)


def factor_kernel(pivot, upper_out, inverse_out, work, diag, upper, inv, panel, parts):
    order = work.shape[0]
    lane = lax.broadcasted_iota(jnp.int32, (BLOCK, order), 1)
    pieces, piece_rows, piece_cols = pivot.shape
    across = order // piece_cols
    for index in range(pieces):
        first_row = index // across * piece_rows
        first_col = index % across * piece_cols
        if first_row < first_col + piece_cols:
            work[pl.ds(first_row, piece_rows), pl.ds(first_col, piece_cols)] = pivot[index]
        else:
            work[pl.ds(first_row, piece_rows), pl.ds(first_col, piece_cols)] = jnp.zeros(
                (piece_rows, piece_cols), jnp.float32
            )

    def finish(start, here, solved):
        inverse_out[here, :] = jnp.where(lane < start + BLOCK, solved, 0.0)
        upper_out[here, :] = jnp.where(lane >= start + BLOCK, solved, 0.0)
        upper_out[here, here] = upper[...]

    factor_steps(work, diag, upper, inv, panel, parts, finish)


def factor(pivot, order):
    spec = pl.BlockSpec(memory_space=pltpu.VMEM)
    shape = jax.ShapeDtypeStruct((order, order), jnp.float32)
    return pl.pallas_call(
        factor_kernel,
        out_shape=(shape, shape),
        in_specs=[spec],
        out_specs=(spec, spec),
        scratch_shapes=[
            pltpu.VMEM((order, order), jnp.float32),
            pltpu.VMEM((BLOCK, BLOCK), jnp.float32),
            pltpu.VMEM((BLOCK, BLOCK), jnp.float32),
            pltpu.VMEM((BLOCK, BLOCK), jnp.float32),
            pltpu.VMEM((BLOCK, order), jnp.float32),
            pltpu.VMEM((3, 2 * BLOCK, order), jnp.bfloat16),
        ],
        compiler_params=pltpu.CompilerParams(vmem_limit_bytes=40 * 2**20),
        cost_estimate=pl.CostEstimate(
            flops=60 * order**3, bytes_accessed=12 * order * order, transcendentals=order
        ),
        name="factor",
    )(pivot)


def flip(value):
    return value + 1 - 2 * (value % 2)


def remote(src, dst, send, recv, target):
    return pltpu.make_async_remote_copy(
        src_ref=src,
        dst_ref=dst,
        send_sem=send,
        recv_sem=recv,
        device_id=target,
        device_id_type=pl.DeviceIdType.MESH,
    )


def piece_needed(row, col, chunk):
    return col >= 2 * row + chunk


def split_pair(value):
    top = value.astype(jnp.bfloat16)
    return top, (value - top.astype(jnp.float32)).astype(jnp.bfloat16)


def dot_t(left, right):
    return lax.dot_general(
        left, right, (((1,), (1,)), ((), ())), preferred_element_type=jnp.float32
    )


def dot_pair(left, right):
    return dot_t(left[0], right[0]) + (dot_t(left[0], right[1]) + dot_t(left[1], right[0]))


def front_kernel(
    pivot, border, update, child_map, parent_diag, pivot_out, border_out, parent_out,
    work, inv_top, inv_low, diag, upper, inv, panel, parts,
    rows_in, cols_in, relay, sent, own, got, sol_top, sol_low, col_top, col_low,
    own_top, own_low, maps, diag_in, hot, total,
    local_sem, psend, precv, fsend, frecv, bsend, brecv, xsend, xrecv, ssend, srecv, osem,
):
    leaf = lax.axis_index("leaf")
    row = lax.axis_index("row")
    col = lax.axis_index("col")
    core = col % 2
    cross = (col + 2) % 4
    mate = flip(col)
    mate_cross = (mate + 2) % 4
    leaf_side = leaf % 2
    on_diag = row == col // 2
    to_mate_id = (leaf, row, mate)
    to_side_id = (leaf, row, cross)
    to_over_id = (leaf, 1 - row, col)
    to_far_id = (leaf, 1 - row, cross)
    sibling_id = (flip(leaf), row, col)

    piece_rows, piece_cols = pivot.shape
    order = work.shape[0]
    rows_local, cols_local = update.shape
    block = rows_local // 2
    chunks, _, width = sent.shape
    step = piece_rows // 2
    half_rows = parent_out.shape[0]
    parent_cols = parent_out.shape[1]
    slots = order // piece_cols

    barrier = pltpu.get_barrier_semaphore()
    for target in (to_mate_id, to_side_id, to_over_id, to_far_id, sibling_id):
        pl.semaphore_signal(
            barrier, inc=1, device_id=target, device_id_type=pl.DeviceIdType.MESH
        )

    def spread(value, size):
        return pl.ds(pl.multiple_of(value * size, size), size)

    sent_part = 1 - leaf_side
    own_part = leaf_side
    here_rows = spread(row, piece_rows)
    here_cols = spread(col, piece_cols)
    keep_pivot = pltpu.make_async_copy(pivot, work.at[here_rows, here_cols], local_sem.at[0])
    keep_border = pltpu.make_async_copy(border, rows_in.at[:, here_cols], local_sem.at[1])
    keep_map = pltpu.make_async_copy(child_map, maps, local_sem.at[2])
    keep_diag = pltpu.make_async_copy(parent_diag, diag_in, local_sem.at[3])
    keep_own = pltpu.make_async_copy(update.at[spread(own_part, block)], own, local_sem.at[4])

    def keep_sent(index):
        return pltpu.make_async_copy(
            update.at[spread(sent_part, block), pl.ds(index * width, width)],
            sent.at[index],
            osem.at[index],
        )

    keep_pivot.start()
    keep_border.start()
    keep_map.start()
    keep_diag.start()
    keep_own.start()
    for index in range(chunks):
        keep_sent(index).start()
    pl.semaphore_wait(barrier, 5)

    targets = (to_over_id, to_side_id, to_far_id, to_mate_id)

    def own_piece(index, chunk):
        there = pl.ds(pl.multiple_of(row * piece_rows + chunk * step, step), step)
        return remote(
            pivot.at[pl.ds(chunk * step, step)], work.at[there, here_cols],
            psend.at[index, chunk], precv.at[index, chunk], targets[index],
        )

    def pass_piece(index, chunk, source_row, source_col):
        there = pl.ds(pl.multiple_of(source_row * piece_rows + chunk * step, step), step)
        where = work.at[there, spread(source_col, piece_cols)]
        return remote(
            where, where, fsend.at[index, chunk], frecv.at[index, chunk], to_mate_id
        )

    for chunk in range(2):
        @pl.when(piece_needed(row, col, chunk))
        def _(chunk=chunk):
            for index in range(4):
                own_piece(index, chunk).start()

    def part_of(index):
        return sent_part if index == 0 else own_part

    def border_to(kind, index, target):
        there = spread(part_of(index), block)
        return remote(
            border.at[there], rows_in.at[there, here_cols],
            bsend.at[kind, index], brecv.at[kind, index], target,
        )

    def pass_side(index):
        where = rows_in.at[spread(part_of(index), block), spread(cross, piece_cols)]
        return remote(where, where, bsend.at[2, index], brecv.at[2, index], to_mate_id)

    core_rows = spread(core, block)

    def to_relay():
        return remote(border.at[core_rows], relay, xsend.at[0, 0], xrecv.at[0, 0], to_over_id)

    def from_relay(index):
        there = pl.ds(index * width, width)
        return remote(
            relay.at[there], cols_in.at[there, here_cols],
            xsend.at[1, index], xrecv.at[1, index], to_side_id,
        )

    def over_first():
        return remote(
            border.at[core_rows], cols_in.at[:, here_cols],
            xsend.at[2, 0], xrecv.at[2, 0], to_over_id,
        )

    def over_mate():
        where = spread(mate, piece_cols)
        return remote(
            rows_in.at[core_rows, where], cols_in.at[:, where],
            xsend.at[3, 0], xrecv.at[3, 0], to_over_id,
        )

    def over_last(index):
        where = spread(mate_cross, piece_cols)
        there = pl.ds(pl.multiple_of(core * block + index * width, width), width)
        return remote(
            rows_in.at[there, where], cols_in.at[pl.ds(index * width, width), where],
            xsend.at[4, index], xrecv.at[4, index], to_over_id,
        )

    for index in range(2):
        border_to(0, index, to_side_id).start()
        border_to(1, index, to_mate_id).start()

    @pl.when(on_diag)
    def _():
        over_first().start()

    @pl.when(jnp.logical_not(on_diag))
    def _():
        to_relay().start()

    remote_slots = ((1 - row, col), (row, cross), (1 - row, cross))
    mate_slots = ((1 - row, mate), (row, mate_cross), (1 - row, mate_cross))
    for chunk in range(2):
        for index, (source_row, source_col) in enumerate(remote_slots):
            @pl.when(piece_needed(source_row, source_col, chunk))
            def _(index=index, chunk=chunk, source_row=source_row, source_col=source_col):
                own_piece(index, chunk).wait_recv()
                pass_piece(index, chunk, source_row, source_col).start()

    for chunk in range(2):
        @pl.when(piece_needed(row, mate, chunk))
        def _(chunk=chunk):
            own_piece(3, chunk).wait_recv()
        for index, (source_row, source_col) in enumerate(mate_slots):
            @pl.when(piece_needed(source_row, source_col, chunk))
            def _(index=index, chunk=chunk):
                pass_piece(index, chunk, row, col).wait_recv()
        for index, (source_row, source_col) in enumerate(remote_slots):
            @pl.when(piece_needed(source_row, source_col, chunk))
            def _(index=index, chunk=chunk):
                pass_piece(index, chunk, row, col).wait_send()
    keep_pivot.wait()

    def pump(kb):
        @pl.when(kb == 1)
        def _():
            keep_border.wait()
            for index in range(2):
                border_to(1, index, to_mate_id).wait_recv()

            @pl.when(on_diag)
            def _():
                over_mate().start()

        @pl.when(kb == 3)
        def _():
            border_to(0, 0, to_side_id).wait_recv()
            pass_side(0).start()

        @pl.when(kb == 4)
        def _():
            @pl.when(on_diag)
            def _():
                to_relay().wait_recv()
                for index in range(chunks):
                    from_relay(index).start()

        @pl.when(kb == 6)
        def _():
            border_to(0, 1, to_side_id).wait_recv()
            pass_side(1).start()

        @pl.when(kb == 7)
        def _():
            for index in range(2):
                pass_side(index).wait_recv()

            @pl.when(on_diag)
            def _():
                for index in range(chunks):
                    over_last(index).start()

    lane = lax.broadcasted_iota(jnp.int32, (BLOCK, order), 1)

    def finish(start, here, solved):
        top, low = split_pair(jnp.where(lane < start + BLOCK, solved, 0.0))
        inv_top[here, :] = top
        inv_low[here, :] = low
        work[here, :] = jnp.where(lane >= start + BLOCK, solved, 0.0)
        work[here, here] = upper[...]

    factor_steps(work, diag, upper, inv, panel, parts, finish, pump)

    def solve_tile(value):
        pair = split_pair(value)
        for slot in range(slots):
            depth = (slot + 1) * piece_cols
            there = pl.ds(slot * piece_cols, piece_cols)
            result = dot_pair(
                (pair[0][:, :depth], pair[1][:, :depth]),
                (inv_top[there, :depth], inv_low[there, :depth]),
            )
            yield slot, there, result

    tile = piece_cols

    def solve_rows(part):
        def body(index, carry):
            source = pl.ds(pl.multiple_of(part * block + index * tile, tile), tile)
            for slot, there, result in solve_tile(rows_in[source, :]):
                top, low = split_pair(result)
                sol_top[pl.ds(pl.multiple_of(index * tile, tile), tile), there] = top
                sol_low[pl.ds(pl.multiple_of(index * tile, tile), tile), there] = low

                @pl.when(col == slot)
                def _(result=result):
                    border_out[source, :] = result
            return carry

        lax.fori_loop(0, block // tile, body, 0)

    solve_rows(sent_part)

    @pl.when(on_diag)
    def _():
        near = pltpu.make_async_copy(rows_in.at[core_rows], cols_in, local_sem.at[5])
        near.start()
        near.wait()

    @pl.when(jnp.logical_not(on_diag))
    def _():
        over_first().wait_recv()
        over_mate().wait_recv()

    def swap(index):
        return remote(
            sent.at[index], got.at[index], ssend.at[index], srecv.at[index], sibling_id
        )

    def send_step(index, carry):
        there = pl.ds(pl.multiple_of(index * width, width), width)

        @pl.when(jnp.logical_not(on_diag))
        def _():
            where = cols_in.at[there, here_cols]
            remote(where, where, xsend.at[1, index], xrecv.at[1, index], to_side_id).wait_recv()
            remote(where, where, xsend.at[4, index], xrecv.at[4, index], to_over_id).wait_recv()

        for slot, place, result in solve_tile(cols_in[there, :]):
            top, low = split_pair(result)
            col_top[there, place] = top
            col_low[there, place] = low
        pltpu.make_async_copy(
            update.at[pl.ds(0, block), pl.ds(0, width)], sent.at[index], osem.at[index]
        ).wait()

        def rows_step(part, carry):
            here = pl.ds(pl.multiple_of(part * tile, tile), tile)
            change = dot_pair(
                (sol_top[here, :], sol_low[here, :]), (col_top[there, :], col_low[there, :])
            )
            sent[index, here, :] = sent[index, here, :] - change
            return carry

        lax.fori_loop(0, block // tile, rows_step, 0)
        swap(index).start()
        return carry

    lax.fori_loop(0, chunks, send_step, 0)

    piece = work[spread(col, piece_cols), spread(row, piece_rows)]
    pivot_out[...] = piece.T

    solve_rows(own_part)
    keep_own.wait()

    def own_step(index, carry):
        here = pl.ds(pl.multiple_of(index * tile, tile), tile)
        for part in range(cols_local // tile):
            there = pl.ds(part * tile, tile)
            change = dot_pair(
                (sol_top[here, :], sol_low[here, :]), (col_top[there, :], col_low[there, :])
            )
            top, low = split_pair(own[here, there] - change)
            own_top[here, there] = top
            own_low[here, there] = low
        return carry

    lax.fori_loop(0, block // tile, own_step, 0)

    keep_map.wait()
    keep_diag.wait()
    row_block = 2 * row + leaf_side
    third = half_rows // 3

    def one_hot_rows(which, owner, position, base):
        def body(index, carry):
            here = pl.ds(pl.multiple_of(index * third, third), third)
            goal = maps[pl.ds(owner, 1), spread(position, block)] - base - index * third
            at = lax.broadcasted_iota(jnp.int32, (third, block), 0)
            hot[which, here, :] = jnp.where(at == goal, 1.0, 0.0).astype(jnp.bfloat16)
            return carry

        lax.fori_loop(0, half_rows // third, body, 0)

    def pick_t(left, right):
        return dot_t(left[0], right) + dot_t(left[1], right)

    def pick(left, right):
        return jnp.dot(left, right[0], preferred_element_type=jnp.float32) + jnp.dot(
            left, right[1], preferred_element_type=jnp.float32
        )

    one_hot_rows(0, leaf, row_block, row_block * half_rows)
    one_hot_rows(1, leaf, col, col * parent_cols)

    def own_place(index, carry):
        here = pl.ds(pl.multiple_of(index * third, third), third)
        wide = split_pair(pick(hot[0, here, :], (own_top[...], own_low[...])))
        for part in range(parent_cols // third):
            there = pl.ds(part * third, third)
            result = pick_t(wide, hot[1, there, :])
            down = lax.broadcasted_iota(jnp.int32, (third, third), 0) + index * third
            across = lax.broadcasted_iota(jnp.int32, (third, third), 1) + part * third
            on_line = (down == across) & (row_block == col)
            total[here, there] = result + jnp.where(on_line, diag_in[0:1, there], 0.0)
        return carry

    lax.fori_loop(0, half_rows // third, own_place, 0)

    one_hot_rows(0, flip(leaf), row_block, row_block * half_rows)
    one_hot_rows(1, flip(leaf), col, col * parent_cols)

    def out_copy(index):
        there = pl.ds(index * width, width)
        return pltpu.make_async_copy(
            total.at[:, there], parent_out.at[:, there], osem.at[chunks + index]
        )

    reach = parent_cols - cols_local
    last = parent_cols // width
    for index in range(chunks):
        swap(index).wait_recv()
        low = index * width
        high = low + width + reach
        arrived = split_pair(got[index])

        def got_step(part, carry, low=low, high=high, arrived=arrived):
            here = pl.ds(pl.multiple_of(part * third, third), third)
            wide = split_pair(pick(hot[0, here, :], arrived))
            result = pick_t(wide, hot[1, pl.ds(low, high - low), pl.ds(low, width)])
            total[here, pl.ds(low, high - low)] = total[here, pl.ds(low, high - low)] + result
            return carry

        lax.fori_loop(0, half_rows // third, got_step, 0)
        for done in range(index, index + 1 if index + 1 < chunks else last):
            out_copy(done).start()

    @pl.when(jnp.logical_not(on_diag))
    def _():
        to_relay().wait_send()

    @pl.when(on_diag)
    def _():
        over_first().wait_send()
        over_mate().wait_send()
        for index in range(chunks):
            from_relay(index).wait_send()
            over_last(index).wait_send()

    for index in range(2):
        border_to(0, index, to_side_id).wait_send()
        border_to(1, index, to_mate_id).wait_send()
        pass_side(index).wait_send()
    for chunk in range(2):
        @pl.when(piece_needed(row, col, chunk))
        def _(chunk=chunk):
            for index in range(4):
                own_piece(index, chunk).wait_send()
    for index in range(chunks):
        swap(index).wait_send()
    for index in range(last):
        out_copy(index).wait()


def whole_front(pivot, border, update, child_map, parent_diag, order):
    piece_rows, piece_cols = pivot.shape
    rows_local, cols_local = update.shape
    block = rows_local // 2
    width = BLOCK
    chunks = cols_local // width
    half_rows = parent_diag.shape[1]
    parent_cols = half_rows
    vmem = pl.BlockSpec(memory_space=pltpu.VMEM)
    anywhere = pl.BlockSpec(memory_space=pl.ANY)
    dma = pltpu.SemaphoreType.DMA
    f32 = jnp.float32
    b16 = jnp.bfloat16
    return pl.pallas_call(
        front_kernel,
        out_shape=(
            jax.ShapeDtypeStruct((piece_rows, piece_cols), f32),
            jax.ShapeDtypeStruct((rows_local, piece_cols), f32),
            jax.ShapeDtypeStruct((half_rows, parent_cols), f32),
        ),
        in_specs=[anywhere] * 5,
        out_specs=(vmem, vmem, anywhere),
        scratch_shapes=[
            pltpu.VMEM((order, order), f32),
            pltpu.VMEM((order, order), b16),
            pltpu.VMEM((order, order), b16),
            pltpu.VMEM((BLOCK, BLOCK), f32),
            pltpu.VMEM((BLOCK, BLOCK), f32),
            pltpu.VMEM((BLOCK, BLOCK), f32),
            pltpu.VMEM((BLOCK, order), f32),
            pltpu.VMEM((3, 2 * BLOCK, order), b16),
            pltpu.VMEM((rows_local, order), f32),
            pltpu.VMEM((block, order), f32),
            pltpu.VMEM((block, piece_cols), f32),
            pltpu.VMEM((chunks, block, width), f32),
            pltpu.VMEM((block, cols_local), f32),
            pltpu.VMEM((chunks, block, width), f32),
            pltpu.VMEM((block, order), b16),
            pltpu.VMEM((block, order), b16),
            pltpu.VMEM((block, order), b16),
            pltpu.VMEM((block, order), b16),
            pltpu.VMEM((block, cols_local), b16),
            pltpu.VMEM((block, cols_local), b16),
            pltpu.VMEM(child_map.shape, jnp.int32),
            pltpu.VMEM(parent_diag.shape, f32),
            pltpu.VMEM((2, half_rows, block), b16),
            pltpu.VMEM((half_rows, parent_cols), f32),
            dma((6,)), dma((4, 2)), dma((4, 2)), dma((3, 2)), dma((3, 2)),
            dma((3, 2)), dma((3, 2)), dma((5, chunks)), dma((5, chunks)),
            dma((chunks,)), dma((chunks,)), dma((chunks + parent_cols // width,)),
        ],
        compiler_params=pltpu.CompilerParams(
            vmem_limit_bytes=62 * 2**20, collective_id=0, has_side_effects=True
        ),
        name="whole_front",
    )(pivot, border, update, child_map, parent_diag)


def high_dot_t(left, right):
    return lax.dot_general(
        left, right, (((1,), (1,)), ((), ())), precision=HIGH, preferred_element_type=jnp.float32
    )


def split_two(value):
    top = lax.reduce_precision(value, 8, 7)
    return top.astype(jnp.bfloat16), (value - top).astype(jnp.bfloat16)


def one_hot(targets, size):
    return (jnp.arange(size, dtype=jnp.int32)[:, None] == targets[None, :]).astype(jnp.bfloat16)


def pick_dot(left, right, dims):
    return lax.dot_general(left, right, (dims, ((), ())), preferred_element_type=jnp.float32)


def place_blocks(blocks, rows_to, cols_to, out_rows, out_cols):
    col_hot = one_hot(cols_to, out_cols)
    first = 0
    placed = None
    for block in blocks:
        count = block.shape[0]
        row_hot = one_hot(rows_to[first : first + count], out_rows)
        first += count
        top, rest = split_two(block)
        wide = pick_dot(top, col_hot, ((1,), (1,))) + pick_dot(rest, col_hot, ((1,), (1,)))
        top, rest = split_two(wide)
        part = pick_dot(row_hot, top, ((1,), (0,))) + pick_dot(row_hot, rest, ((1,), (0,)))
        placed = part if placed is None else placed + part
    return placed


def column_border(bord, full_rows, nrow, ncol, cols_local, row_index, col_index):
    rows_local, width = bord.shape
    if nrow == 2 and rows_local % cols_local == 0:
        per_row = rows_local // cols_local
        mine = lax.dynamic_slice_in_dim(full_rows, (col_index % per_row) * cols_local, cols_local, 0)
        received = jnp.zeros((cols_local, full_rows.shape[1]), bord.dtype)
        for shift in range(ncol):
            pairs = []
            for c in range(ncol):
                home = c // per_row
                pairs.append((home * ncol + (c + shift) % ncol, (1 - home) * ncol + c))
            target = (col_index - shift + ncol) % ncol
            part = lax.dynamic_slice_in_dim(bord, (target % per_row) * cols_local, cols_local, 0)
            moved = lax.ppermute(part, ("row", "col"), pairs)
            place = (col_index + shift) % ncol * width
            received = lax.dynamic_update_slice_in_dim(received, moved, place, 1)
        return jnp.where(row_index == col_index // per_row, mine, received)
    whole = lax.all_gather(full_rows, "row", axis=0, tiled=True)
    return lax.dynamic_slice_in_dim(whole, col_index * cols_local, cols_local, 0)


def fits(nrow, ncol, pivot, border, update, child_map, parent_diag):
    rows, cols = update.shape
    half_rows = parent_diag.shape[1]
    return (
        nrow == 2
        and ncol == 4
        and pivot.shape[0] == 2 * pivot.shape[1]
        and rows == 2 * cols
        and border.shape == (rows, pivot.shape[1])
        and child_map.shape[1] == nrow * rows
        and pivot.shape[1] % (2 * BLOCK) == 0
        and cols % pivot.shape[1] == 0
        and half_rows % (3 * BLOCK) == 0
        and half_rows > cols
    )


def on_device(pivot, border, update, child_map, parent_diag):
    nrow = lax.axis_size("row")
    ncol = lax.axis_size("col")
    row_index = lax.axis_index("row")
    col_index = lax.axis_index("col")
    leaf_index = lax.axis_index("leaf")
    piece = pivot[0]
    piece_rows, piece_cols = piece.shape
    if fits(nrow, ncol, piece, border[0], update[0], child_map, parent_diag):
        order = nrow * piece_rows
        outs = whole_front(piece, border[0], update[0], child_map, parent_diag, order)
        return tuple(out[None] for out in outs)
    stacked = lax.all_gather(piece[None], ("row", "col"), axis=0, tiled=True)
    stacked, bord = lax.optimization_barrier((stacked, border[0]))
    upper, inverse = factor(stacked, nrow * piece_rows)
    pivot_out = lax.dynamic_slice(
        upper, (col_index * piece_cols, row_index * piece_rows), (piece_cols, piece_rows)
    ).T

    rows_local = bord.shape[0]
    trailing = update[0]
    cols_local = trailing.shape[1]
    full_rows = lax.all_gather(bord, "col", axis=1, tiled=True)
    col_rows = column_border(bord, full_rows, nrow, ncol, cols_local, row_index, col_index)
    factor_cols = high_dot_t(col_rows, inverse)

    half_rows = parent_diag.shape[1]
    block_rows = 2 * half_rows
    parent_cols = block_rows * nrow // ncol
    side = leaf_index % 2
    partner = leaf_index + 1 - 2 * side
    total_cols = child_map.shape[1]
    own_map = lax.dynamic_slice(child_map, (leaf_index, 0), (1, total_cols))[0]
    partner_map = lax.dynamic_slice(child_map, (partner, 0), (1, total_cols))[0]
    swap = [(source, source ^ 1) for source in range(lax.axis_size("leaf"))]

    map_block = total_cols // max(nrow, ncol)
    halves = rows_local % (2 * map_block) == 0
    if halves:
        kept = rows_local // 2
        own_start = side * kept
        sent_start = (1 - side) * kept

        def schur_rows(start, size):
            rows = lax.dynamic_slice_in_dim(full_rows, start, size, 0)
            below = high_dot_t(rows, inverse)
            part = lax.dynamic_slice_in_dim(trailing, start, size, 0)
            return below, part - high_dot_t(below, factor_cols)

        sent_parts = []
        sibling = []
        chunk = kept // CHUNKS
        for index in range(CHUNKS):
            below, sent = schur_rows(sent_start + index * chunk, chunk)
            sent_parts.append(below)
            sibling.append(lax.ppermute(sent, "leaf", swap))
        sent_below = jnp.concatenate(sent_parts, axis=0)
        own_below, own = schur_rows(own_start, kept)
        own_slice = lax.dynamic_slice_in_dim(own_below, col_index * piece_cols, piece_cols, 1)
        sent_slice = lax.dynamic_slice_in_dim(sent_below, col_index * piece_cols, piece_cols, 1)
        border_out = jnp.where(
            side == 0,
            jnp.concatenate([own_slice, sent_slice], axis=0),
            jnp.concatenate([sent_slice, own_slice], axis=0),
        )
    else:
        kept = rows_local
        own_start = 0
        factor_rows = high_dot_t(full_rows, inverse)
        own = trailing - high_dot_t(factor_rows, factor_cols)
        sibling = [lax.ppermute(own, "leaf", swap)]
        border_out = lax.dynamic_slice_in_dim(factor_rows, col_index * piece_cols, piece_cols, 1)

    def my_half(blocks, mapping):
        rows_to = (
            lax.dynamic_slice_in_dim(mapping, row_index * rows_local + own_start, kept)
            - row_index * block_rows
            - side * half_rows
        )
        cols_to = (
            lax.dynamic_slice_in_dim(mapping, col_index * cols_local, cols_local)
            - col_index * parent_cols
        )
        return place_blocks(blocks, rows_to, cols_to, half_rows, parent_cols)

    global_rows = row_index * block_rows + side * half_rows + jnp.arange(half_rows, dtype=jnp.int32)
    global_cols = col_index * parent_cols + jnp.arange(parent_cols, dtype=jnp.int32)
    diagonal = jnp.where(global_rows[:, None] == global_cols[None, :], parent_diag[0][:, None], 0.0)
    parent_out = my_half([own], own_map) + diagonal + my_half(sibling, partner_map)
    return (pivot_out[None], border_out[None], parent_out[None])


def solution(mesh):
    placed = (
        P("leaf", "row", "col"),
        P("leaf", "row", "col"),
        P("leaf", "row", "col"),
        P(),
        P("leaf", "row"),
    )
    return jax.shard_map(
        on_device,
        mesh=mesh,
        in_specs=placed,
        out_specs=(P("leaf", "row", "col"), P("leaf", "row", "col"), P("leaf", "row", "col")),
        check_vma=False,
    )
```

```python
import jax
import jax.numpy as jnp
from jax import lax
from jax.experimental import pallas as pl
from jax.experimental.pallas import tpu as pltpu
from jax.sharding import PartitionSpec as P

BLOCK = 128
CHUNKS = 2
PANEL = 8
HIGH = lax.Precision.HIGH


def exact_dot(left, right):
    return jnp.dot(left, right, precision=lax.Precision.HIGHEST, preferred_element_type=jnp.float32)


def factor_small(entry):
    work = {key: value for key, value in entry.items()}
    lower = {}
    inverse = {}
    for k in range(PANEL):
        scale = lax.rsqrt(work[k, k])
        for i in range(k + 1, PANEL):
            lower[i, k] = work[i, k] * scale
        for j in range(k + 1, PANEL):
            for i in range(j, PANEL):
                work[i, j] = work[i, j] - lower[i, k] * lower[j, k]
        inverse[k, k] = scale
        for j in range(k):
            total = lower[k, j] * inverse[j, j]
            for m in range(j + 1, k):
                total = total + lower[k, m] * inverse[m, j]
            inverse[k, j] = -(total * scale)
    return inverse


def factor_block(diag, upper, inv):
    lane8 = lax.broadcasted_iota(jnp.int32, (PANEL, BLOCK), 1)
    lane_all = lax.broadcasted_iota(jnp.int32, (BLOCK, BLOCK), 1)

    def panel_step(p, carry):
        base = p * PANEL
        start = pl.multiple_of(base, PANEL)
        rows = diag[pl.ds(start, PANEL), :]
        full = diag[...]
        entry = {}
        for b in range(PANEL):
            index = jnp.zeros((PANEL, BLOCK), jnp.int32) + (base + b)
            col = jnp.take_along_axis(rows, index, axis=1, mode="promise_in_bounds")
            for a in range(b, PANEL):
                entry[a, b] = jnp.broadcast_to(col[a : a + 1, :], (PANEL, BLOCK))
        inverse = factor_small(entry)
        inside = (lane8 >= base) & (lane8 < base + PANEL)
        plain = []
        augmented = []
        for k in range(PANEL):
            row = jnp.broadcast_to(rows[k : k + 1, :], (PANEL, BLOCK))
            plain.append(row)
            augmented.append(jnp.where(inside, (lane8 == base + k).astype(jnp.float32), row))
        solved = []
        for a in range(PANEL):
            up = inverse[a, 0] * plain[0]
            au = inverse[a, 0] * augmented[0]
            for k in range(1, a + 1):
                up = up + inverse[a, k] * plain[k]
                au = au + inverse[a, k] * augmented[k]
            solved.append(au)
            keep = lane8 >= base + a
            upper[pl.ds(start + a, 1), :] = jnp.where(keep, up, 0.0)[0:1, :]
            inv[pl.ds(start + a, 1), :] = jnp.where(lane8 <= base + a, au, 0.0)[0:1, :]
        inside_all = (lane_all >= base) & (lane_all < base + PANEL)
        trailing = jnp.where(inside_all, 0.0, full)
        for m in range(PANEL):
            gain = inverse[m, m] * solved[m]
            for a in range(m + 1, PANEL):
                gain = gain + inverse[a, m] * solved[a]
            index = jnp.zeros((BLOCK, BLOCK), jnp.int32) + (base + m)
            col = jnp.take_along_axis(full, index, axis=1, mode="promise_in_bounds")
            trailing = trailing - col * jnp.broadcast_to(gain[0:1, :], (BLOCK, BLOCK))
        diag[...] = trailing
        return carry

    lax.fori_loop(0, BLOCK // PANEL, panel_step, 0)


def split_three(value):
    top = value.astype(jnp.bfloat16)
    rest = value - top.astype(jnp.float32)
    mid = rest.astype(jnp.bfloat16)
    return top, mid, (rest - mid.astype(jnp.float32)).astype(jnp.bfloat16)


def factor_steps(work, diag, upper, inv, panel, parts, finish, pump=None):
    order = work.shape[0]
    count = order // BLOCK

    def block_step(kb, carry):
        if pump is not None:
            pump(kb)
        start = pl.multiple_of(kb * BLOCK, BLOCK)
        here = pl.ds(start, BLOCK)
        diag[...] = work[here, here]
        factor_block(diag, upper, inv)
        work[here, here] = jnp.where(
            lax.broadcasted_iota(jnp.int32, (BLOCK, BLOCK), 0)
            == lax.broadcasted_iota(jnp.int32, (BLOCK, BLOCK), 1),
            1.0,
            0.0,
        )
        panel[...] = exact_dot(inv[...], work[here, :])
        solved = panel[...]
        finish(start, here, solved)

        top, mid, low = split_three(solved)
        parts[0, :BLOCK, :] = top
        parts[0, BLOCK:, :] = top
        parts[1, :BLOCK, :] = mid
        parts[1, BLOCK:, :] = mid
        parts[2, :BLOCK, :] = low
        parts[2, BLOCK:, :] = top

        def row_step(ib, carry):
            there = pl.ds(pl.multiple_of(ib * BLOCK, BLOCK), BLOCK)
            top, mid, low = split_three(panel[:, there].T)
            both = jnp.concatenate([top, mid], axis=1)
            ends = jnp.concatenate([top, low], axis=1)
            change = jnp.dot(ends, parts[2], preferred_element_type=jnp.float32)
            change = change + jnp.dot(both, parts[1], preferred_element_type=jnp.float32)
            change = change + jnp.dot(both, parts[0], preferred_element_type=jnp.float32)
            work[there, here] = jnp.zeros((BLOCK, BLOCK), jnp.float32)
            work[there, :] = work[there, :] - change
            return carry

        lax.fori_loop(kb + 1, count, row_step, 0)
        return carry

    lax.fori_loop(0, count, block_step, 0)


def factor_kernel(pivot, upper_out, inverse_out, work, diag, upper, inv, panel, parts):
    order = work.shape[0]
    lane = lax.broadcasted_iota(jnp.int32, (BLOCK, order), 1)
    pieces, piece_rows, piece_cols = pivot.shape
    across = order // piece_cols
    for index in range(pieces):
        first_row = index // across * piece_rows
        first_col = index % across * piece_cols
        if first_row < first_col + piece_cols:
            work[pl.ds(first_row, piece_rows), pl.ds(first_col, piece_cols)] = pivot[index]
        else:
            work[pl.ds(first_row, piece_rows), pl.ds(first_col, piece_cols)] = jnp.zeros(
                (piece_rows, piece_cols), jnp.float32
            )

    def finish(start, here, solved):
        inverse_out[here, :] = jnp.where(lane < start + BLOCK, solved, 0.0)
        upper_out[here, :] = jnp.where(lane >= start + BLOCK, solved, 0.0)
        upper_out[here, here] = upper[...]

    factor_steps(work, diag, upper, inv, panel, parts, finish)


def factor(pivot, order):
    spec = pl.BlockSpec(memory_space=pltpu.VMEM)
    shape = jax.ShapeDtypeStruct((order, order), jnp.float32)
    return pl.pallas_call(
        factor_kernel,
        out_shape=(shape, shape),
        in_specs=[spec],
        out_specs=(spec, spec),
        scratch_shapes=[
            pltpu.VMEM((order, order), jnp.float32),
            pltpu.VMEM((BLOCK, BLOCK), jnp.float32),
            pltpu.VMEM((BLOCK, BLOCK), jnp.float32),
            pltpu.VMEM((BLOCK, BLOCK), jnp.float32),
            pltpu.VMEM((BLOCK, order), jnp.float32),
            pltpu.VMEM((3, 2 * BLOCK, order), jnp.bfloat16),
        ],
        compiler_params=pltpu.CompilerParams(vmem_limit_bytes=40 * 2**20),
        cost_estimate=pl.CostEstimate(
            flops=60 * order**3, bytes_accessed=12 * order * order, transcendentals=order
        ),
        name="factor",
    )(pivot)


def flip(value):
    return value + 1 - 2 * (value % 2)


def remote(src, dst, send, recv, target):
    return pltpu.make_async_remote_copy(
        src_ref=src,
        dst_ref=dst,
        send_sem=send,
        recv_sem=recv,
        device_id=target,
        device_id_type=pl.DeviceIdType.MESH,
    )


def lane_column(rows, place):
    index = jnp.full(rows.shape, place, jnp.int32)
    return jnp.take_along_axis(rows, index, axis=1, mode="promise_in_bounds")


def factor_diagonal(diag, upper, inv):
    lane = lax.broadcasted_iota(jnp.int32, (PANEL, BLOCK), 1)
    count = BLOCK // PANEL
    rows = [diag[pl.ds(index * PANEL, PANEL), :] for index in range(count)]
    for step in range(count):
        base = step * PANEL
        entry = {}
        for b in range(PANEL):
            column = lane_column(rows[step], base + b)
            for a in range(b, PANEL):
                entry[a, b] = jnp.broadcast_to(column[a : a + 1, :], (PANEL, BLOCK))
        inverse = factor_small(entry)
        inside = (lane >= base) & (lane < base + PANEL)
        plain = []
        augmented = []
        for k in range(PANEL):
            line = jnp.broadcast_to(rows[step][k : k + 1, :], (PANEL, BLOCK))
            plain.append(line)
            augmented.append(jnp.where(inside, (lane == base + k).astype(jnp.float32), line))
        solved = []
        for a in range(PANEL):
            up = inverse[a, 0] * plain[0]
            au = inverse[a, 0] * augmented[0]
            for k in range(1, a + 1):
                up = up + inverse[a, k] * plain[k]
                au = au + inverse[a, k] * augmented[k]
            solved.append(au)
            upper[pl.ds(base + a, 1), :] = jnp.where(lane >= base + a, up, 0.0)[0:1, :]
            inv[pl.ds(base + a, 1), :] = jnp.where(lane <= base + a, au, 0.0)[0:1, :]
        if step + 1 == count:
            break
        gains = []
        for m in range(PANEL):
            gain = inverse[m, m] * solved[m]
            for a in range(m + 1, PANEL):
                gain = gain + inverse[a, m] * solved[a]
            gains.append(gain)
        for later in range(step + 1, count):
            value = jnp.where(inside, 0.0, rows[later])
            for m in range(PANEL):
                value = value - lane_column(rows[later], base + m) * gains[m]
            rows[later] = value


def six_pass(left, parts):
    top, mid, low = split_three(left)
    both = jnp.concatenate([top, mid], axis=1)
    ends = jnp.concatenate([top, low], axis=1)
    change = jnp.dot(ends, parts[2], preferred_element_type=jnp.float32)
    change = change + jnp.dot(both, parts[1], preferred_element_type=jnp.float32)
    return change + jnp.dot(both, parts[0], preferred_element_type=jnp.float32)


def store_parts(parts, value):
    top, mid, low = split_three(value)
    parts[0, :BLOCK, :] = top
    parts[0, BLOCK:, :] = top
    parts[1, :BLOCK, :] = mid
    parts[1, BLOCK:, :] = mid
    parts[2, :BLOCK, :] = low
    parts[2, BLOCK:, :] = top


def split_pair(value):
    top = value.astype(jnp.bfloat16)
    return top, (value - top.astype(jnp.float32)).astype(jnp.bfloat16)


def dot_t(left, right):
    return lax.dot_general(
        left, right, (((1,), (1,)), ((), ())), preferred_element_type=jnp.float32
    )


def dot_pair(left, right):
    return dot_t(left[0], right[0]) + (dot_t(left[0], right[1]) + dot_t(left[1], right[0]))


def front_kernel(
    pivot, border, update, child_map, parent_diag, pivot_out, border_out, parent_out,
    work, inv_top, inv_low, diag, upper, inv, parts, pool,
    rows_in, cols_in, relay, sent, own, got, fill, maps, diag_in, hot,
    local_sem, psend, precv, fsend, frecv, bsend, brecv, xsend, xrecv, ssend, srecv, osem,
    tsend, trecv,
):
    leaf = lax.axis_index("leaf")
    row = lax.axis_index("row")
    col = lax.axis_index("col")
    core = col % 2
    cross = (col + 2) % 4
    mate = flip(col)
    mate_cross = (mate + 2) % 4
    leaf_side = leaf % 2
    on_diag = row == col // 2
    off_diag = jnp.logical_not(on_diag)
    to_mate_id = (leaf, row, mate)
    to_side_id = (leaf, row, cross)
    to_over_id = (leaf, 1 - row, col)
    to_far_id = (leaf, 1 - row, cross)
    sibling_id = (flip(leaf), row, col)

    piece_rows, piece_cols = pivot.shape
    order = work.shape[0]
    rows_local, cols_local = update.shape
    block = rows_local // 2
    chunks, _, width = sent.shape
    pieces = piece_rows // BLOCK
    half_rows = parent_out.shape[0]
    parent_cols = parent_out.shape[1]
    slots = order // piece_cols
    count = order // BLOCK

    barrier = pltpu.get_barrier_semaphore()
    for target in (to_mate_id, to_side_id, to_over_id, to_far_id, sibling_id):
        pl.semaphore_signal(
            barrier, inc=1, device_id=target, device_id_type=pl.DeviceIdType.MESH
        )

    def spread(value, size):
        return pl.ds(pl.multiple_of(value * size, size), size)

    sent_part = 1 - leaf_side
    own_part = leaf_side
    here_rows = spread(row, piece_rows)
    here_cols = spread(col, piece_cols)
    keep_pivot = pltpu.make_async_copy(pivot, work.at[here_rows, here_cols], local_sem.at[0])
    keep_border = pltpu.make_async_copy(border, rows_in.at[:, here_cols], local_sem.at[1])
    keep_map = pltpu.make_async_copy(child_map, maps, local_sem.at[2])
    keep_diag = pltpu.make_async_copy(parent_diag, diag_in, local_sem.at[3])
    keep_own = pltpu.make_async_copy(update.at[spread(own_part, block)], own, local_sem.at[4])

    def keep_sent(index):
        return pltpu.make_async_copy(
            update.at[spread(sent_part, block), pl.ds(index * width, width)],
            sent.at[index],
            osem.at[index],
        )

    keep_pivot.start()
    keep_border.start()
    keep_map.start()
    keep_diag.start()
    pair = 2 * BLOCK
    rows_top = pool.at[pl.ds(0, order)]
    rows_mid = pool.at[pl.ds(order, order)]
    rows_low = pool.at[pl.ds(2 * order, order)]

    def clear_step(index, carry):
        there = pl.ds(pl.multiple_of(index * BLOCK, BLOCK), BLOCK)
        for rows in (rows_top, rows_mid, rows_low):
            rows[there, :] = jnp.zeros((BLOCK, order), jnp.bfloat16)
        return carry

    lax.fori_loop(0, count, clear_step, 0)
    pl.semaphore_wait(barrier, 5)

    targets = (to_over_id, to_side_id, to_far_id, to_mate_id)
    remote_slots = ((1 - row, col), (row, cross), (1 - row, cross))
    mate_slots = ((1 - row, mate), (row, mate_cross), (1 - row, mate_cross))

    def piece_needed(source_row, source_col, chunk):
        return (source_col + 1) * (piece_cols // BLOCK) > source_row * pieces + chunk

    def own_piece(index, chunk):
        there = pl.ds(pl.multiple_of(row * piece_rows + chunk * BLOCK, BLOCK), BLOCK)
        return remote(
            pivot.at[pl.ds(chunk * BLOCK, BLOCK)], work.at[there, here_cols],
            psend.at[index, chunk], precv.at[index, chunk], targets[index],
        )

    def pass_piece(index, chunk, source_row, source_col):
        there = pl.ds(pl.multiple_of(source_row * piece_rows + chunk * BLOCK, BLOCK), BLOCK)
        where = work.at[there, spread(source_col, piece_cols)]
        return remote(
            where, where, fsend.at[index, chunk], frecv.at[index, chunk], to_mate_id
        )

    for chunk in range(pieces):
        @pl.when(piece_needed(row, col, chunk))
        def _(chunk=chunk):
            for index in range(4):
                own_piece(index, chunk).start()

    def part_of(index):
        return sent_part if index == 0 else own_part

    def border_to(kind, index, target):
        there = spread(part_of(index), block)
        return remote(
            border.at[there], rows_in.at[there, here_cols],
            bsend.at[kind, index], brecv.at[kind, index], target,
        )

    def pass_side(index):
        where = rows_in.at[spread(part_of(index), block), spread(cross, piece_cols)]
        return remote(where, where, bsend.at[2, index], brecv.at[2, index], to_mate_id)

    core_rows = spread(core, block)

    def group_rows(index):
        return pl.ds(pl.multiple_of(core * block + index * width, width), width)

    def to_relay(index):
        return remote(
            border.at[group_rows(index)], relay.at[pl.ds(index * width, width)],
            xsend.at[0, index], xrecv.at[0, index], to_over_id,
        )

    def from_relay(index):
        there = pl.ds(index * width, width)
        return remote(
            relay.at[there], cols_in.at[there, here_cols],
            xsend.at[1, index], xrecv.at[1, index], to_side_id,
        )

    def over_first(index):
        return remote(
            border.at[group_rows(index)], cols_in.at[pl.ds(index * width, width), here_cols],
            xsend.at[2, index], xrecv.at[2, index], to_over_id,
        )

    def over_slot(kind, which, index):
        where = spread(which, piece_cols)
        return remote(
            rows_in.at[group_rows(index), where], cols_in.at[pl.ds(index * width, width), where],
            xsend.at[kind, index], xrecv.at[kind, index], to_over_id,
        )

    def over_mate(index):
        return over_slot(3, mate, index)

    def over_last(index):
        return over_slot(4, mate_cross, index)

    border_to(0, 0, to_side_id).start()
    for index in range(2):
        border_to(1, index, to_mate_id).start()

    @pl.when(on_diag)
    def _():
        for index in range(chunks):
            over_first(index).start()

    @pl.when(off_diag)
    def _():
        for index in range(chunks):
            to_relay(index).start()
        border_to(0, 1, to_side_id).start()

    def forward_row(source_row, chunk, pick=lambda which: True):
        for index, (from_row, from_col) in enumerate(remote_slots):
            chosen = (from_row == source_row) & pick(from_col)

            @pl.when(chosen & piece_needed(from_row, from_col, chunk))
            def _(index=index, from_row=from_row, from_col=from_col):
                own_piece(index, chunk).wait_recv()
                pass_piece(index, chunk, from_row, from_col).start()

    def collect_row(source_row, chunk, pick=lambda which: True):
        @pl.when((row == source_row) & pick(mate) & piece_needed(row, mate, chunk))
        def _():
            own_piece(3, chunk).wait_recv()
        for index, (from_row, from_col) in enumerate(mate_slots):
            chosen = (from_row == source_row) & pick(from_col)

            @pl.when(chosen & piece_needed(from_row, from_col, chunk))
            def _(index=index):
                pass_piece(index, chunk, row, col).wait_recv()
        for index, (from_row, from_col) in enumerate(remote_slots):
            chosen = (from_row == source_row) & pick(from_col)

            @pl.when(chosen & piece_needed(from_row, from_col, chunk))
            def _(index=index):
                pass_piece(index, chunk, row, col).wait_send()

    def is_first(which):
        return which == 0

    def is_later(which):
        return which > 0

    def pump_before(kb):
        @pl.when(kb == 0)
        def _():
            keep_pivot.wait()
            forward_row(0, 0, is_first)
            collect_row(0, 0, is_first)
        for step in range(1, count):
            @pl.when(kb == step)
            def _(step=step):
                collect_row(step // pieces, step % pieces)

    def pump_after(kb):
        @pl.when(kb == 0)
        def _():
            forward_row(0, 0, is_later)
            collect_row(0, 0, is_later)
        for step in range(count - 1):
            @pl.when(kb == step)
            def _(step=step):
                forward_row((step + 1) // pieces, (step + 1) % pieces)

        @pl.when(kb == 0)
        def _():
            keep_own.start()
            for index in range(chunks):
                keep_sent(index).start()

        @pl.when(kb == 1)
        def _():
            keep_border.wait()
            for index in range(2):
                border_to(1, index, to_mate_id).wait_recv()

            @pl.when(on_diag)
            def _():
                for index in range(chunks):
                    over_mate(index).start()

        @pl.when((kb == 3) & on_diag)
        def _():
            for index in range(chunks - 1):
                to_relay(index).wait_recv()
                from_relay(index).start()

        @pl.when((kb == 4) & on_diag)
        def _():
            to_relay(chunks - 1).wait_recv()
            from_relay(chunks - 1).start()
            border_to(0, 1, to_side_id).start()

        @pl.when(kb == 5)
        def _():
            border_to(0, 0, to_side_id).wait_recv()
            pass_side(0).start()

        @pl.when(kb == 6)
        def _():
            pass_side(0).wait_recv()

            @pl.when(on_diag & (core == sent_part))
            def _():
                for index in range(chunks):
                    over_last(index).start()

        @pl.when((kb == 7) & on_diag)
        def _():
            border_to(0, 1, to_side_id).wait_recv()
            pass_side(1).start()

    lane = lax.broadcasted_iota(jnp.int32, (BLOCK, order), 1)

    pair_lane = lax.broadcasted_iota(jnp.int32, (BLOCK, pair), 1)


    def block_step(kb, carry):
        pump_before(kb)
        start = pl.multiple_of(kb * BLOCK, BLOCK)
        here = pl.ds(start, BLOCK)

        def past_step(past, carry):
            there = pl.ds(pl.multiple_of(past * pair, pair), pair)
            known = pair_lane + past * pair < start
            top, mid, low = split_three(jnp.where(known, work[there, here].T, 0.0))
            work[here, there] = jnp.where(known, 0.0, work[here, there])
            first = jnp.dot(
                jnp.concatenate([top, mid, low], axis=0), rows_top[there, :],
                preferred_element_type=jnp.float32,
            )
            second = jnp.dot(
                jnp.concatenate([top, mid], axis=0), rows_mid[there, :],
                preferred_element_type=jnp.float32,
            )
            third = jnp.dot(top, rows_low[there, :], preferred_element_type=jnp.float32)
            small = (first[2 * BLOCK :] + third) + second[BLOCK:]
            change = first[:BLOCK] + ((first[BLOCK:pair] + second[:BLOCK]) + small)
            work[here, :] = work[here, :] - change
            return carry

        lax.fori_loop(0, (kb + 1) // 2, past_step, 0)

        @pl.when(kb % 2 == 1)
        def _():
            before = pl.ds(pl.multiple_of((kb - kb % 2) * BLOCK, BLOCK), BLOCK)
            for rows in (rows_top, rows_mid, rows_low):
                rows[before, here] = jnp.zeros((BLOCK, BLOCK), jnp.bfloat16)

        diag[...] = work[here, here]
        factor_diagonal(diag, upper, inv)
        pump_after(kb)
        work[here, here] = jnp.where(
            lax.broadcasted_iota(jnp.int32, (BLOCK, BLOCK), 0)
            == lax.broadcasted_iota(jnp.int32, (BLOCK, BLOCK), 1),
            1.0,
            0.0,
        )
        store_parts(parts, work[here, :])
        solved = six_pass(inv[...], [parts[index] for index in range(3)])
        low_part = jnp.where(lane < start + BLOCK, solved, 0.0)
        top, low = split_pair(low_part)
        inv_top[here, :] = top
        inv_low[here, :] = low
        work[here, :] = jnp.where(lane >= start + BLOCK, solved, 0.0)
        work[here, here] = upper[...]
        top, mid, low = split_three(solved)
        rows_top[here, :] = top
        rows_mid[here, :] = mid
        rows_low[here, :] = low
        return carry

    lax.fori_loop(0, count, block_step, 0)

    sol_top = pool.at[pl.ds(0, block)]
    sol_low = pool.at[pl.ds(block, block)]
    col_top = pool.at[pl.ds(2 * block, block)]
    col_low = pool.at[pl.ds(3 * block, block)]
    own_top = pool.at[pl.ds(4 * block, block), pl.ds(0, cols_local)]
    own_low = pool.at[pl.ds(5 * block, block), pl.ds(0, cols_local)]
    raw_top = pool.at[pl.ds(6 * block, block)]
    raw_low = pool.at[pl.ds(7 * block, block)]

    def solve_slots(left_top, left_low):
        for slot in range(slots):
            depth = (slot + 1) * piece_cols
            there = pl.ds(slot * piece_cols, piece_cols)
            result = dot_pair(
                (left_top[:, :depth], left_low[:, :depth]),
                (inv_top[there, :depth], inv_low[there, :depth]),
            )
            yield slot, there, result

    def solve_rows(part):
        def body(index, carry):
            source = pl.ds(pl.multiple_of(part * block + index * width, width), width)
            goal = pl.ds(pl.multiple_of(index * width, width), width)
            top, low = split_pair(rows_in[source, :])
            raw_top[goal, :] = top
            raw_low[goal, :] = low
            return carry

        lax.fori_loop(0, block // width, body, 0)
        for slot, there, result in solve_slots(raw_top, raw_low):
            top, low = split_pair(result)
            sol_top[:, there] = top
            sol_low[:, there] = low

            @pl.when(col == slot)
            def _(result=result):
                border_out[spread(part, block), :] = result

    @pl.when(on_diag)
    def _():
        pass_side(1).wait_recv()

        @pl.when(core != sent_part)
        def _():
            for index in range(chunks):
                over_last(index).start()

    solve_rows(sent_part)

    @pl.when(on_diag)
    def _():
        near = pltpu.make_async_copy(rows_in.at[core_rows], cols_in, local_sem.at[5])
        near.start()
        near.wait()

    def swap(index, thin):
        there = pl.ds(index * width if thin else 0, block - index * width if thin else block)
        return remote(
            sent.at[index, there], got.at[index, there],
            ssend.at[index], srecv.at[index], sibling_id,
        )

    def share(index, later):
        return remote(
            got.at[index, pl.ds(later * width, width)], fill.at[index, later],
            tsend.at[index, later], trecv.at[index, later], to_far_id,
        )

    thin_send = core == sent_part
    thin_get = core == own_part

    def by_kind(thin, action):
        @pl.when(thin)
        def _():
            action(True)

        @pl.when(jnp.logical_not(thin))
        def _():
            action(False)

    def arrive(index):
        by_kind(thin_get, lambda thin: swap(index, thin).wait_recv())

        @pl.when(thin_get & off_diag)
        def _():
            for later in range(index + 1, chunks):
                share(index, later).start()

    def complete(index):
        for before in range(index):
            goal = pl.ds(before * width, width)

            @pl.when(thin_get & off_diag)
            def _(before=before, goal=goal):
                share(before, index).wait_recv()
                got[index, goal, :] = fill[before, index].T

            @pl.when(thin_get & on_diag)
            def _(before=before, goal=goal):
                got[index, goal, :] = got[before, pl.ds(index * width, width), :].T

    def send_step(index, carry):
        there = pl.ds(pl.multiple_of(index * width, width), width)

        @pl.when(off_diag)
        def _():
            where = cols_in.at[there, here_cols]
            for kind, target in ((1, to_side_id), (2, to_over_id), (3, to_over_id), (4, to_over_id)):
                remote(
                    where, where, xsend.at[kind, index], xrecv.at[kind, index], target
                ).wait_recv()

        top, low = split_pair(cols_in[there, :])
        for slot, place, result in solve_slots(top, low):
            top_part, low_part = split_pair(result)
            col_top[there, place] = top_part
            col_low[there, place] = low_part
        pltpu.make_async_copy(
            update.at[pl.ds(0, block), pl.ds(0, width)], sent.at[index], osem.at[index]
        ).wait()
        change = dot_pair(
            (sol_top[...], sol_low[...]), (col_top[there, :], col_low[there, :])
        )
        sent[index] = sent[index] - change
        for which in range(chunks):
            @pl.when(index == which)
            def _(which=which):
                by_kind(thin_send, lambda thin: swap(which, thin).start())
        return carry

    lax.fori_loop(0, chunks, send_step, 0)

    piece = work[spread(col, piece_cols), spread(row, piece_rows)]
    pivot_out[...] = piece.T

    @pl.when(off_diag)
    def _():
        border_to(0, 1, to_side_id).wait_recv()
        pass_side(1).start()
        pass_side(1).wait_recv()

    solve_rows(own_part)
    keep_own.wait()
    for part in range(cols_local // width):
        there = pl.ds(part * width, width)
        change = dot_pair(
            (sol_top[...], sol_low[...]), (col_top[there, :], col_low[there, :])
        )
        top, low = split_pair(own[:, there] - change)
        own_top[:, there] = top
        own_low[:, there] = low

    keep_map.wait()
    keep_diag.wait()
    row_block = 2 * row + leaf_side
    third = half_rows // 3
    slack = half_rows - block

    def one_hot_rows(which, owner, position, base):
        def body(index, carry):
            here = pl.ds(pl.multiple_of(index * third, third), third)
            goal = maps[pl.ds(owner, 1), spread(position, block)] - base - index * third
            at = lax.broadcasted_iota(jnp.int32, (third, block), 0)
            hot[which, here, :] = jnp.where(at == goal, 1.0, 0.0).astype(jnp.bfloat16)
            return carry

        lax.fori_loop(0, half_rows // third, body, 0)

    def pick_t(left, right):
        return dot_t(left[0], right) + dot_t(left[1], right)

    def pick(left, right):
        return jnp.dot(left, right[0], preferred_element_type=jnp.float32) + jnp.dot(
            left, right[1], preferred_element_type=jnp.float32
        )

    def band(index):
        first = max(0, index * third - slack) // BLOCK * BLOCK
        return pl.ds(first, min(block, -(-(index + 1) * third // BLOCK) * BLOCK) - first)

    arrive(0)
    one_hot_rows(0, leaf, row_block, row_block * half_rows)
    one_hot_rows(1, leaf, col, col * parent_cols)

    for index in range(3):
        here = pl.ds(index * third, third)
        rows = band(index)
        wide = split_pair(pick(hot[0, here, rows], (own_top[rows, :], own_low[rows, :])))
        raw_top[pl.ds(0, third), pl.ds(0, cols_local)] = wide[0]
        raw_low[pl.ds(0, third), pl.ds(0, cols_local)] = wide[1]
        for part in range(3):
            there = pl.ds(part * third, third)
            cols = band(part)
            result = pick_t(
                (raw_top[pl.ds(0, third), cols], raw_low[pl.ds(0, third), cols]),
                hot[1, there, cols],
            )
            if index == part:
                down = lax.broadcasted_iota(jnp.int32, (third, third), 0)
                across = lax.broadcasted_iota(jnp.int32, (third, third), 1)
                on_line = (down == across) & (row_block == col)
                result = result + jnp.where(on_line, diag_in[0:1, there], 0.0)
            parent_out[here, there] = result

    one_hot_rows(0, flip(leaf), row_block, row_block * half_rows)
    one_hot_rows(1, flip(leaf), col, col * parent_cols)

    for index in range(chunks):
        if index > 0:
            arrive(index)
        complete(index)
        low = index * width
        there = pl.ds(low, width + slack)
        arrived = split_pair(got[index])
        raw_top[:, pl.ds(0, width)] = arrived[0]
        raw_low[:, pl.ds(0, width)] = arrived[1]
        for part in range(3):
            here = pl.ds(part * third, third)
            rows = band(part)
            wide = split_pair(
                pick(hot[0, here, rows], (raw_top[rows, pl.ds(0, width)], raw_low[rows, pl.ds(0, width)]))
            )
            result = pick_t(wide, hot[1, there, pl.ds(low, width)])
            parent_out[here, there] = parent_out[here, there] + result

    @pl.when(off_diag)
    def _():
        for index in range(chunks):
            to_relay(index).wait_send()

    @pl.when(on_diag)
    def _():
        for index in range(chunks):
            from_relay(index).wait_send()
            over_first(index).wait_send()
            over_mate(index).wait_send()
            over_last(index).wait_send()

    for index in range(2):
        border_to(0, index, to_side_id).wait_send()
        border_to(1, index, to_mate_id).wait_send()
        pass_side(index).wait_send()
    for chunk in range(pieces):
        @pl.when(piece_needed(row, col, chunk))
        def _(chunk=chunk):
            for index in range(4):
                own_piece(index, chunk).wait_send()
    for index in range(chunks):
        by_kind(thin_send, lambda thin: swap(index, thin).wait_send())

    @pl.when(thin_get & off_diag)
    def _():
        for index in range(chunks):
            for later in range(index + 1, chunks):
                share(index, later).wait_send()


def store_kernel(*refs):
    copies = [
        pltpu.make_async_copy(refs[index], refs[3 + index], refs[6].at[index])
        for index in range(3)
    ]
    for copy in copies:
        copy.start()
    for copy in copies:
        copy.wait()


def whole_front(pivot, border, update, child_map, parent_diag, order):
    piece_rows, piece_cols = pivot.shape
    rows_local, cols_local = update.shape
    block = rows_local // 2
    width = piece_cols
    chunks = cols_local // width
    steps = order // BLOCK
    pool_rows = max(steps * 6 * BLOCK, 8 * block)
    pieces = piece_rows // BLOCK
    half_rows = parent_diag.shape[1]
    parent_cols = half_rows
    vmem = pl.BlockSpec(memory_space=pltpu.VMEM)
    anywhere = pl.BlockSpec(memory_space=pl.ANY)
    dma = pltpu.SemaphoreType.DMA
    f32 = jnp.float32
    b16 = jnp.bfloat16
    results = pl.pallas_call(
        front_kernel,
        out_shape=(
            pltpu.VMEM((piece_rows, piece_cols), f32),
            pltpu.VMEM((rows_local, piece_cols), f32),
            pltpu.VMEM((half_rows, parent_cols), f32),
        ),
        in_specs=[pl.BlockSpec(memory_space=pltpu.HBM)] * 5,
        out_specs=(vmem, vmem, vmem),
        scratch_shapes=[
            pltpu.VMEM((order, order), f32),
            pltpu.VMEM((order, order), b16),
            pltpu.VMEM((order, order), b16),
            pltpu.VMEM((BLOCK, BLOCK), f32),
            pltpu.VMEM((BLOCK, BLOCK), f32),
            pltpu.VMEM((BLOCK, BLOCK), f32),
            pltpu.VMEM((3, 2 * BLOCK, order), b16),
            pltpu.VMEM((pool_rows, order), b16),
            pltpu.VMEM((rows_local, order), f32),
            pltpu.VMEM((block, order), f32),
            pltpu.VMEM((block, piece_cols), f32),
            pltpu.VMEM((chunks, block, width), f32),
            pltpu.VMEM((block, cols_local), f32),
            pltpu.VMEM((chunks, block, width), f32),
            pltpu.VMEM((chunks, chunks, width, width), f32),
            pltpu.VMEM(child_map.shape, jnp.int32),
            pltpu.VMEM(parent_diag.shape, f32),
            pltpu.VMEM((2, half_rows, block), b16),
            dma((6,)), dma((4, pieces)), dma((4, pieces)), dma((3, pieces)), dma((3, pieces)),
            dma((3, 2)), dma((3, 2)), dma((5, chunks)), dma((5, chunks)),
            dma((chunks,)), dma((chunks,)), dma((chunks,)),
            dma((chunks, chunks)), dma((chunks, chunks)),
        ],
        compiler_params=pltpu.CompilerParams(
            vmem_limit_bytes=56 * 2**20, collective_id=0, has_side_effects=True
        ),
        name="whole_front",
    )(pivot, border, update, child_map, parent_diag)
    return pl.pallas_call(
        store_kernel,
        out_shape=tuple(jax.ShapeDtypeStruct(result.shape, f32) for result in results),
        in_specs=[vmem] * 3,
        out_specs=(pl.BlockSpec(memory_space=pltpu.HBM),) * 3,
        scratch_shapes=[dma((3,))],
        compiler_params=pltpu.CompilerParams(vmem_limit_bytes=2**20),
        name="store_results",
    )(*results)


def high_dot_t(left, right):
    return lax.dot_general(
        left, right, (((1,), (1,)), ((), ())), precision=HIGH, preferred_element_type=jnp.float32
    )


def split_two(value):
    top = lax.reduce_precision(value, 8, 7)
    return top.astype(jnp.bfloat16), (value - top).astype(jnp.bfloat16)


def one_hot(targets, size):
    return (jnp.arange(size, dtype=jnp.int32)[:, None] == targets[None, :]).astype(jnp.bfloat16)


def pick_dot(left, right, dims):
    return lax.dot_general(left, right, (dims, ((), ())), preferred_element_type=jnp.float32)


def place_blocks(blocks, rows_to, cols_to, out_rows, out_cols):
    col_hot = one_hot(cols_to, out_cols)
    first = 0
    placed = None
    for block in blocks:
        count = block.shape[0]
        row_hot = one_hot(rows_to[first : first + count], out_rows)
        first += count
        top, rest = split_two(block)
        wide = pick_dot(top, col_hot, ((1,), (1,))) + pick_dot(rest, col_hot, ((1,), (1,)))
        top, rest = split_two(wide)
        part = pick_dot(row_hot, top, ((1,), (0,))) + pick_dot(row_hot, rest, ((1,), (0,)))
        placed = part if placed is None else placed + part
    return placed


def column_border(bord, full_rows, nrow, ncol, cols_local, row_index, col_index):
    rows_local, width = bord.shape
    if nrow == 2 and rows_local % cols_local == 0:
        per_row = rows_local // cols_local
        mine = lax.dynamic_slice_in_dim(full_rows, (col_index % per_row) * cols_local, cols_local, 0)
        received = jnp.zeros((cols_local, full_rows.shape[1]), bord.dtype)
        for shift in range(ncol):
            pairs = []
            for c in range(ncol):
                home = c // per_row
                pairs.append((home * ncol + (c + shift) % ncol, (1 - home) * ncol + c))
            target = (col_index - shift + ncol) % ncol
            part = lax.dynamic_slice_in_dim(bord, (target % per_row) * cols_local, cols_local, 0)
            moved = lax.ppermute(part, ("row", "col"), pairs)
            place = (col_index + shift) % ncol * width
            received = lax.dynamic_update_slice_in_dim(received, moved, place, 1)
        return jnp.where(row_index == col_index // per_row, mine, received)
    whole = lax.all_gather(full_rows, "row", axis=0, tiled=True)
    return lax.dynamic_slice_in_dim(whole, col_index * cols_local, cols_local, 0)


def fits(nrow, ncol, pivot, border, update, child_map, parent_diag):
    rows, cols = update.shape
    half_rows = parent_diag.shape[1]
    return (
        nrow == 2
        and ncol == 4
        and pivot.shape[0] == 2 * pivot.shape[1]
        and rows == 2 * cols
        and border.shape == (rows, pivot.shape[1])
        and child_map.shape[1] == nrow * rows
        and pivot.shape[1] % (2 * BLOCK) == 0
        and cols % pivot.shape[1] == 0
        and half_rows % (3 * BLOCK) == 0
        and half_rows > cols
    )


def on_device(pivot, border, update, child_map, parent_diag):
    nrow = lax.axis_size("row")
    ncol = lax.axis_size("col")
    row_index = lax.axis_index("row")
    col_index = lax.axis_index("col")
    leaf_index = lax.axis_index("leaf")
    piece = pivot[0]
    piece_rows, piece_cols = piece.shape
    if fits(nrow, ncol, piece, border[0], update[0], child_map, parent_diag):
        order = nrow * piece_rows
        outs = whole_front(piece, border[0], update[0], child_map, parent_diag, order)
        return tuple(out[None] for out in outs)
    stacked = lax.all_gather(piece[None], ("row", "col"), axis=0, tiled=True)
    stacked, bord = lax.optimization_barrier((stacked, border[0]))
    upper, inverse = factor(stacked, nrow * piece_rows)
    pivot_out = lax.dynamic_slice(
        upper, (col_index * piece_cols, row_index * piece_rows), (piece_cols, piece_rows)
    ).T

    rows_local = bord.shape[0]
    trailing = update[0]
    cols_local = trailing.shape[1]
    full_rows = lax.all_gather(bord, "col", axis=1, tiled=True)
    col_rows = column_border(bord, full_rows, nrow, ncol, cols_local, row_index, col_index)
    factor_cols = high_dot_t(col_rows, inverse)

    half_rows = parent_diag.shape[1]
    block_rows = 2 * half_rows
    parent_cols = block_rows * nrow // ncol
    side = leaf_index % 2
    partner = leaf_index + 1 - 2 * side
    total_cols = child_map.shape[1]
    own_map = lax.dynamic_slice(child_map, (leaf_index, 0), (1, total_cols))[0]
    partner_map = lax.dynamic_slice(child_map, (partner, 0), (1, total_cols))[0]
    swap = [(source, source ^ 1) for source in range(lax.axis_size("leaf"))]

    map_block = total_cols // max(nrow, ncol)
    halves = rows_local % (2 * map_block) == 0
    if halves:
        kept = rows_local // 2
        own_start = side * kept
        sent_start = (1 - side) * kept

        def schur_rows(start, size):
            rows = lax.dynamic_slice_in_dim(full_rows, start, size, 0)
            below = high_dot_t(rows, inverse)
            part = lax.dynamic_slice_in_dim(trailing, start, size, 0)
            return below, part - high_dot_t(below, factor_cols)

        sent_parts = []
        sibling = []
        chunk = kept // CHUNKS
        for index in range(CHUNKS):
            below, sent = schur_rows(sent_start + index * chunk, chunk)
            sent_parts.append(below)
            sibling.append(lax.ppermute(sent, "leaf", swap))
        sent_below = jnp.concatenate(sent_parts, axis=0)
        own_below, own = schur_rows(own_start, kept)
        own_slice = lax.dynamic_slice_in_dim(own_below, col_index * piece_cols, piece_cols, 1)
        sent_slice = lax.dynamic_slice_in_dim(sent_below, col_index * piece_cols, piece_cols, 1)
        border_out = jnp.where(
            side == 0,
            jnp.concatenate([own_slice, sent_slice], axis=0),
            jnp.concatenate([sent_slice, own_slice], axis=0),
        )
    else:
        kept = rows_local
        own_start = 0
        factor_rows = high_dot_t(full_rows, inverse)
        own = trailing - high_dot_t(factor_rows, factor_cols)
        sibling = [lax.ppermute(own, "leaf", swap)]
        border_out = lax.dynamic_slice_in_dim(factor_rows, col_index * piece_cols, piece_cols, 1)

    def my_half(blocks, mapping):
        rows_to = (
            lax.dynamic_slice_in_dim(mapping, row_index * rows_local + own_start, kept)
            - row_index * block_rows
            - side * half_rows
        )
        cols_to = (
            lax.dynamic_slice_in_dim(mapping, col_index * cols_local, cols_local)
            - col_index * parent_cols
        )
        return place_blocks(blocks, rows_to, cols_to, half_rows, parent_cols)

    global_rows = row_index * block_rows + side * half_rows + jnp.arange(half_rows, dtype=jnp.int32)
    global_cols = col_index * parent_cols + jnp.arange(parent_cols, dtype=jnp.int32)
    diagonal = jnp.where(global_rows[:, None] == global_cols[None, :], parent_diag[0][:, None], 0.0)
    parent_out = my_half([own], own_map) + diagonal + my_half(sibling, partner_map)
    return (pivot_out[None], border_out[None], parent_out[None])


def solution(mesh):
    placed = (
        P("leaf", "row", "col"),
        P("leaf", "row", "col"),
        P("leaf", "row", "col"),
        P(),
        P("leaf", "row"),
    )
    return jax.shard_map(
        on_device,
        mesh=mesh,
        in_specs=placed,
        out_specs=(P("leaf", "row", "col"), P("leaf", "row", "col"), P("leaf", "row", "col")),
        check_vma=False,
    )
```

```python
import jax
import jax.numpy as jnp
from jax import lax
from jax.experimental import pallas as pl
from jax.experimental.pallas import tpu as pltpu
from jax.sharding import PartitionSpec as P

BLOCK = 128
CHUNKS = 2
PANEL = 8
HIGH = lax.Precision.HIGH


def exact_dot(left, right):
    return jnp.dot(left, right, precision=lax.Precision.HIGHEST, preferred_element_type=jnp.float32)


def factor_small(entry):
    work = {key: value for key, value in entry.items()}
    lower = {}
    inverse = {}
    for k in range(PANEL):
        scale = lax.rsqrt(work[k, k])
        for i in range(k + 1, PANEL):
            lower[i, k] = work[i, k] * scale
        for j in range(k + 1, PANEL):
            for i in range(j, PANEL):
                work[i, j] = work[i, j] - lower[i, k] * lower[j, k]
        inverse[k, k] = scale
        for j in range(k):
            total = lower[k, j] * inverse[j, j]
            for m in range(j + 1, k):
                total = total + lower[k, m] * inverse[m, j]
            inverse[k, j] = -(total * scale)
    return inverse


def factor_block(diag, upper, inv):
    lane8 = lax.broadcasted_iota(jnp.int32, (PANEL, BLOCK), 1)
    lane_all = lax.broadcasted_iota(jnp.int32, (BLOCK, BLOCK), 1)

    def panel_step(p, carry):
        base = p * PANEL
        start = pl.multiple_of(base, PANEL)
        rows = diag[pl.ds(start, PANEL), :]
        full = diag[...]
        entry = {}
        for b in range(PANEL):
            index = jnp.zeros((PANEL, BLOCK), jnp.int32) + (base + b)
            col = jnp.take_along_axis(rows, index, axis=1, mode="promise_in_bounds")
            for a in range(b, PANEL):
                entry[a, b] = jnp.broadcast_to(col[a : a + 1, :], (PANEL, BLOCK))
        inverse = factor_small(entry)
        inside = (lane8 >= base) & (lane8 < base + PANEL)
        plain = []
        augmented = []
        for k in range(PANEL):
            row = jnp.broadcast_to(rows[k : k + 1, :], (PANEL, BLOCK))
            plain.append(row)
            augmented.append(jnp.where(inside, (lane8 == base + k).astype(jnp.float32), row))
        solved = []
        for a in range(PANEL):
            up = inverse[a, 0] * plain[0]
            au = inverse[a, 0] * augmented[0]
            for k in range(1, a + 1):
                up = up + inverse[a, k] * plain[k]
                au = au + inverse[a, k] * augmented[k]
            solved.append(au)
            keep = lane8 >= base + a
            upper[pl.ds(start + a, 1), :] = jnp.where(keep, up, 0.0)[0:1, :]
            inv[pl.ds(start + a, 1), :] = jnp.where(lane8 <= base + a, au, 0.0)[0:1, :]
        inside_all = (lane_all >= base) & (lane_all < base + PANEL)
        trailing = jnp.where(inside_all, 0.0, full)
        for m in range(PANEL):
            gain = inverse[m, m] * solved[m]
            for a in range(m + 1, PANEL):
                gain = gain + inverse[a, m] * solved[a]
            index = jnp.zeros((BLOCK, BLOCK), jnp.int32) + (base + m)
            col = jnp.take_along_axis(full, index, axis=1, mode="promise_in_bounds")
            trailing = trailing - col * jnp.broadcast_to(gain[0:1, :], (BLOCK, BLOCK))
        diag[...] = trailing
        return carry

    lax.fori_loop(0, BLOCK // PANEL, panel_step, 0)


def split_three(value):
    top = value.astype(jnp.bfloat16)
    rest = value - top.astype(jnp.float32)
    mid = rest.astype(jnp.bfloat16)
    return top, mid, (rest - mid.astype(jnp.float32)).astype(jnp.bfloat16)


def factor_steps(work, diag, upper, inv, panel, parts, finish, pump=None):
    order = work.shape[0]
    count = order // BLOCK

    def block_step(kb, carry):
        if pump is not None:
            pump(kb)
        start = pl.multiple_of(kb * BLOCK, BLOCK)
        here = pl.ds(start, BLOCK)
        diag[...] = work[here, here]
        factor_block(diag, upper, inv)
        work[here, here] = jnp.where(
            lax.broadcasted_iota(jnp.int32, (BLOCK, BLOCK), 0)
            == lax.broadcasted_iota(jnp.int32, (BLOCK, BLOCK), 1),
            1.0,
            0.0,
        )
        panel[...] = exact_dot(inv[...], work[here, :])
        solved = panel[...]
        finish(start, here, solved)

        top, mid, low = split_three(solved)
        parts[0, :BLOCK, :] = top
        parts[0, BLOCK:, :] = top
        parts[1, :BLOCK, :] = mid
        parts[1, BLOCK:, :] = mid
        parts[2, :BLOCK, :] = low
        parts[2, BLOCK:, :] = top

        def row_step(ib, carry):
            there = pl.ds(pl.multiple_of(ib * BLOCK, BLOCK), BLOCK)
            top, mid, low = split_three(panel[:, there].T)
            both = jnp.concatenate([top, mid], axis=1)
            ends = jnp.concatenate([top, low], axis=1)
            change = jnp.dot(ends, parts[2], preferred_element_type=jnp.float32)
            change = change + jnp.dot(both, parts[1], preferred_element_type=jnp.float32)
            change = change + jnp.dot(both, parts[0], preferred_element_type=jnp.float32)
            work[there, here] = jnp.zeros((BLOCK, BLOCK), jnp.float32)
            work[there, :] = work[there, :] - change
            return carry

        lax.fori_loop(kb + 1, count, row_step, 0)
        return carry

    lax.fori_loop(0, count, block_step, 0)


def factor_kernel(pivot, upper_out, inverse_out, work, diag, upper, inv, panel, parts):
    order = work.shape[0]
    lane = lax.broadcasted_iota(jnp.int32, (BLOCK, order), 1)
    pieces, piece_rows, piece_cols = pivot.shape
    across = order // piece_cols
    for index in range(pieces):
        first_row = index // across * piece_rows
        first_col = index % across * piece_cols
        if first_row < first_col + piece_cols:
            work[pl.ds(first_row, piece_rows), pl.ds(first_col, piece_cols)] = pivot[index]
        else:
            work[pl.ds(first_row, piece_rows), pl.ds(first_col, piece_cols)] = jnp.zeros(
                (piece_rows, piece_cols), jnp.float32
            )

    def finish(start, here, solved):
        inverse_out[here, :] = jnp.where(lane < start + BLOCK, solved, 0.0)
        upper_out[here, :] = jnp.where(lane >= start + BLOCK, solved, 0.0)
        upper_out[here, here] = upper[...]

    factor_steps(work, diag, upper, inv, panel, parts, finish)


def factor(pivot, order):
    spec = pl.BlockSpec(memory_space=pltpu.VMEM)
    shape = jax.ShapeDtypeStruct((order, order), jnp.float32)
    return pl.pallas_call(
        factor_kernel,
        out_shape=(shape, shape),
        in_specs=[spec],
        out_specs=(spec, spec),
        scratch_shapes=[
            pltpu.VMEM((order, order), jnp.float32),
            pltpu.VMEM((BLOCK, BLOCK), jnp.float32),
            pltpu.VMEM((BLOCK, BLOCK), jnp.float32),
            pltpu.VMEM((BLOCK, BLOCK), jnp.float32),
            pltpu.VMEM((BLOCK, order), jnp.float32),
            pltpu.VMEM((3, 2 * BLOCK, order), jnp.bfloat16),
        ],
        compiler_params=pltpu.CompilerParams(vmem_limit_bytes=40 * 2**20),
        cost_estimate=pl.CostEstimate(
            flops=60 * order**3, bytes_accessed=12 * order * order, transcendentals=order
        ),
        name="factor",
    )(pivot)


def flip(value):
    return value + 1 - 2 * (value % 2)


def remote(src, dst, send, recv, target):
    return pltpu.make_async_remote_copy(
        src_ref=src,
        dst_ref=dst,
        send_sem=send,
        recv_sem=recv,
        device_id=target,
        device_id_type=pl.DeviceIdType.MESH,
    )


def lane_column(rows, place):
    index = jnp.full(rows.shape, place, jnp.int32)
    return jnp.take_along_axis(rows, index, axis=1, mode="promise_in_bounds")


def factor_diagonal(diag, upper, inv):
    lane = lax.broadcasted_iota(jnp.int32, (PANEL, BLOCK), 1)
    count = BLOCK // PANEL
    rows = [diag[pl.ds(index * PANEL, PANEL), :] for index in range(count)]
    for step in range(count):
        base = step * PANEL
        entry = {}
        for b in range(PANEL):
            column = lane_column(rows[step], base + b)
            for a in range(b, PANEL):
                entry[a, b] = jnp.broadcast_to(column[a : a + 1, :], (PANEL, BLOCK))
        inverse = factor_small(entry)
        inside = (lane >= base) & (lane < base + PANEL)
        plain = []
        augmented = []
        for k in range(PANEL):
            line = jnp.broadcast_to(rows[step][k : k + 1, :], (PANEL, BLOCK))
            plain.append(line)
            augmented.append(jnp.where(inside, (lane == base + k).astype(jnp.float32), line))
        solved = []
        for a in range(PANEL):
            up = inverse[a, 0] * plain[0]
            au = inverse[a, 0] * augmented[0]
            for k in range(1, a + 1):
                up = up + inverse[a, k] * plain[k]
                au = au + inverse[a, k] * augmented[k]
            solved.append(au)
            upper[pl.ds(base + a, 1), :] = jnp.where(lane >= base + a, up, 0.0)[0:1, :]
            inv[pl.ds(base + a, 1), :] = jnp.where(lane <= base + a, au, 0.0)[0:1, :]
        if step + 1 == count:
            break
        gains = []
        for m in range(PANEL):
            gain = inverse[m, m] * solved[m]
            for a in range(m + 1, PANEL):
                gain = gain + inverse[a, m] * solved[a]
            gains.append(gain)
        for later in range(step + 1, count):
            value = jnp.where(inside, 0.0, rows[later])
            for m in range(PANEL):
                value = value - lane_column(rows[later], base + m) * gains[m]
            rows[later] = value


def six_pass(left, parts):
    top, mid, low = split_three(left)
    both = jnp.concatenate([top, mid], axis=1)
    ends = jnp.concatenate([top, low], axis=1)
    change = jnp.dot(ends, parts[2], preferred_element_type=jnp.float32)
    change = change + jnp.dot(both, parts[1], preferred_element_type=jnp.float32)
    return change + jnp.dot(both, parts[0], preferred_element_type=jnp.float32)


def store_parts(parts, value):
    top, mid, low = split_three(value)
    parts[0, :BLOCK, :] = top
    parts[0, BLOCK:, :] = top
    parts[1, :BLOCK, :] = mid
    parts[1, BLOCK:, :] = mid
    parts[2, :BLOCK, :] = low
    parts[2, BLOCK:, :] = top


def split_pair(value):
    top = value.astype(jnp.bfloat16)
    return top, (value - top.astype(jnp.float32)).astype(jnp.bfloat16)


def dot_t(left, right):
    return lax.dot_general(
        left, right, (((1,), (1,)), ((), ())), preferred_element_type=jnp.float32
    )


def dot_pair(left, right):
    return dot_t(left[0], right[0]) + (dot_t(left[0], right[1]) + dot_t(left[1], right[0]))


def front_kernel(
    pivot, border, update, child_map, parent_diag, pivot_out, border_out, parent_out,
    work, inv_top, inv_low, diag, upper, inv, parts, rows_top, rows_mid, rows_low,
    sol_top, sol_low, sol_full, col_top, col_low, own_low,
    rows_in, cols_in, relay, sent, own, got, fill, maps, diag_in, hot,
    local_sem, psend, precv, fsend, frecv, bsend, brecv, xsend, xrecv, ssend, srecv, osem,
    tsend, trecv, hsend, hrecv, gsend, grecv,
):
    leaf = lax.axis_index("leaf")
    row = lax.axis_index("row")
    col = lax.axis_index("col")
    core = col % 2
    cross = (col + 2) % 4
    mate = flip(col)
    mate_cross = (mate + 2) % 4
    leaf_side = leaf % 2
    on_diag = row == col // 2
    off_diag = jnp.logical_not(on_diag)
    to_mate_id = (leaf, row, mate)
    to_side_id = (leaf, row, cross)
    to_over_id = (leaf, 1 - row, col)
    to_far_id = (leaf, 1 - row, cross)
    sibling_id = (flip(leaf), row, col)

    piece_rows, piece_cols = pivot.shape
    order = work.shape[0]
    rows_local, cols_local = update.shape
    block = rows_local // 2
    chunks, _, width = sent.shape
    pieces = piece_rows // BLOCK
    half_rows = parent_out.shape[0]
    parent_cols = parent_out.shape[1]
    slots = order // piece_cols
    count = order // BLOCK

    barrier = pltpu.get_barrier_semaphore()
    for target in (to_mate_id, to_side_id, to_over_id, to_far_id, sibling_id):
        pl.semaphore_signal(
            barrier, inc=1, device_id=target, device_id_type=pl.DeviceIdType.MESH
        )

    def spread(value, size):
        return pl.ds(pl.multiple_of(value * size, size), size)

    sent_part = 1 - leaf_side
    own_part = leaf_side
    here_rows = spread(row, piece_rows)
    here_cols = spread(col, piece_cols)
    keep_pivot = pltpu.make_async_copy(pivot, work.at[here_rows, here_cols], local_sem.at[0])
    keep_border = pltpu.make_async_copy(border, rows_in.at[:, here_cols], local_sem.at[1])
    keep_map = pltpu.make_async_copy(child_map, maps, local_sem.at[2])
    keep_diag = pltpu.make_async_copy(parent_diag, diag_in, local_sem.at[3])
    keep_own = pltpu.make_async_copy(update.at[spread(own_part, block)], own, local_sem.at[4])

    def keep_sent(index):
        return pltpu.make_async_copy(
            update.at[spread(sent_part, block), pl.ds(index * width, width)],
            sent.at[index],
            osem.at[index],
        )

    keep_pivot.start()
    keep_border.start()
    keep_map.start()
    keep_diag.start()
    pair = 2 * BLOCK

    def clear_step(index, carry):
        there = pl.ds(pl.multiple_of(index * BLOCK, BLOCK), BLOCK)
        for rows in (rows_top, rows_mid, rows_low):
            rows[there, :] = jnp.zeros((BLOCK, order), jnp.bfloat16)
        return carry

    lax.fori_loop(0, count, clear_step, 0)
    pl.semaphore_wait(barrier, 5)

    targets = (to_over_id, to_side_id, to_far_id, to_mate_id)
    remote_slots = ((1 - row, col), (row, cross), (1 - row, cross))
    mate_slots = ((1 - row, mate), (row, mate_cross), (1 - row, mate_cross))

    def piece_needed(source_row, source_col, chunk):
        return (source_col + 1) * (piece_cols // BLOCK) > source_row * pieces + chunk

    def own_piece(index, chunk):
        there = pl.ds(pl.multiple_of(row * piece_rows + chunk * BLOCK, BLOCK), BLOCK)
        return remote(
            pivot.at[pl.ds(chunk * BLOCK, BLOCK)], work.at[there, here_cols],
            psend.at[index, chunk], precv.at[index, chunk], targets[index],
        )

    def pass_piece(index, chunk, source_row, source_col):
        there = pl.ds(pl.multiple_of(source_row * piece_rows + chunk * BLOCK, BLOCK), BLOCK)
        where = work.at[there, spread(source_col, piece_cols)]
        return remote(
            where, where, fsend.at[index, chunk], frecv.at[index, chunk], to_mate_id
        )

    below = row > col // 2

    def own_below():
        where = work.at[here_rows, here_cols]
        return remote(pivot, where, psend.at[3, 0], precv.at[3, 0], to_mate_id)

    @pl.when(below)
    def _():
        own_below().start()

    for chunk in range(pieces):
        @pl.when(piece_needed(row, col, chunk))
        def _(chunk=chunk):
            for index in (0, 1, 3):
                own_piece(index, chunk).start()

            @pl.when(on_diag & (row == 0))
            def _():
                own_piece(2, chunk).start()

    def part_of(index):
        return sent_part if index == 0 else own_part

    def border_to(kind, index, target):
        there = spread(part_of(index), block)
        return remote(
            border.at[there], rows_in.at[there, here_cols],
            bsend.at[kind, index], brecv.at[kind, index], target,
        )

    def pass_side(index):
        where = rows_in.at[spread(part_of(index), block), spread(cross, piece_cols)]
        return remote(where, where, bsend.at[2, index], brecv.at[2, index], to_mate_id)

    core_rows = spread(core, block)

    def group_rows(index):
        return pl.ds(pl.multiple_of(core * block + index * width, width), width)

    def to_relay(index):
        return remote(
            border.at[group_rows(index)], relay.at[pl.ds(index * width, width)],
            xsend.at[0, index], xrecv.at[0, index], to_over_id,
        )

    def from_relay(index):
        there = pl.ds(index * width, width)
        return remote(
            relay.at[there], cols_in.at[there, here_cols],
            xsend.at[1, index], xrecv.at[1, index], to_side_id,
        )

    def over_first(index):
        return remote(
            border.at[group_rows(index)], cols_in.at[pl.ds(index * width, width), here_cols],
            xsend.at[2, index], xrecv.at[2, index], to_over_id,
        )

    def over_slot(kind, which, index):
        where = spread(which, piece_cols)
        return remote(
            rows_in.at[group_rows(index), where], cols_in.at[pl.ds(index * width, width), where],
            xsend.at[kind, index], xrecv.at[kind, index], to_over_id,
        )

    def over_mate(index):
        return over_slot(3, mate, index)

    def over_last(index):
        return over_slot(4, mate_cross, index)

    def own_group(kind, index, which, target):
        there = pl.ds(pl.multiple_of(own_part * block + index * width, width), width)
        where = rows_in.at[there, spread(which, piece_cols)]
        source = border.at[there] if kind == 0 else where
        return remote(source, where, gsend.at[kind, index], grecv.at[kind, index], target)

    def side_group(index):
        return own_group(0, index, col, to_side_id)

    def pass_group(index):
        return own_group(1, index, cross, to_mate_id)

    @pl.when(jnp.logical_not(below))
    def _():
        border_to(0, 0, to_side_id).start()

    for index in range(2):
        border_to(1, index, to_mate_id).start()

    @pl.when(on_diag)
    def _():
        over_first(0).start()

    for chunk in range(pieces):
        @pl.when(on_diag & (row == 1) & piece_needed(row, col, chunk))
        def _(chunk=chunk):
            own_piece(2, chunk).start()

    @pl.when(on_diag)
    def _():
        for index in range(1, chunks):
            over_first(index).start()

    @pl.when(off_diag)
    def _():
        for index in range(chunks):
            to_relay(index).start()

    @pl.when(off_diag & jnp.logical_not(below))
    def _():
        for index in range(chunks):
            side_group(index).start()

    def forward_row(source_row, chunk, pick=lambda which: True):
        for index, (from_row, from_col) in enumerate(remote_slots):
            chosen = (from_row == source_row) & pick(from_col)
            if index == 2:
                chosen = chosen & (from_row == from_col // 2)

            @pl.when(chosen & piece_needed(from_row, from_col, chunk))
            def _(index=index, from_row=from_row, from_col=from_col):
                own_piece(index, chunk).wait_recv()
                pass_piece(index, chunk, from_row, from_col).start()

    def collect_row(source_row, chunk, pick=lambda which: True):
        @pl.when((row == source_row) & pick(mate) & piece_needed(row, mate, chunk))
        def _():
            own_piece(3, chunk).wait_recv()
        for index, (from_row, from_col) in enumerate(mate_slots):
            chosen = (from_row == source_row) & pick(from_col)
            if index == 2:
                chosen = chosen & (from_row == from_col // 2)

            @pl.when(chosen & piece_needed(from_row, from_col, chunk))
            def _(index=index):
                pass_piece(index, chunk, row, col).wait_recv()
        for index, (from_row, from_col) in enumerate(remote_slots):
            chosen = (from_row == source_row) & pick(from_col)
            if index == 2:
                chosen = chosen & (from_row == from_col // 2)

            @pl.when(chosen & piece_needed(from_row, from_col, chunk))
            def _(index=index):
                pass_piece(index, chunk, row, col).wait_send()

    def is_first(which):
        return which == 0

    def is_later(which):
        return which > 0

    def pump_before(kb):
        @pl.when(kb == 0)
        def _():
            keep_pivot.wait()

            @pl.when(below)
            def _():
                own_below().wait_recv()
                for which in range(2):
                    value = work[pl.ds(piece_rows, piece_rows), pl.ds(which * piece_cols, piece_cols)]
                    work[pl.ds(which * piece_cols, piece_cols), pl.ds(piece_rows, piece_rows)] = value.T

            forward_row(0, 0, is_first)
            collect_row(0, 0, is_first)
        for step in range(1, count):
            @pl.when(kb == step)
            def _(step=step):
                collect_row(step // pieces, step % pieces)

    def pump_after(kb):
        @pl.when(kb == 0)
        def _():
            forward_row(0, 0, is_later)
            collect_row(0, 0, is_later)
        for step in range(count - 1):
            @pl.when(kb == step)
            def _(step=step):
                forward_row((step + 1) // pieces, (step + 1) % pieces)

        @pl.when(kb == 0)
        def _():
            keep_own.start()
            for index in range(chunks):
                keep_sent(index).start()

        @pl.when(kb == 1)
        def _():
            keep_border.wait()
            for index in range(2):
                border_to(1, index, to_mate_id).wait_recv()

            @pl.when(on_diag)
            def _():
                for index in range(chunks):
                    over_mate(index).start()

        @pl.when((kb == 1) & below)
        def _():
            border_to(0, 0, to_side_id).start()
            for index in range(chunks):
                side_group(index).start()

        @pl.when((kb == 3) & on_diag)
        def _():
            for index in range(chunks - 1):
                to_relay(index).wait_recv()
                from_relay(index).start()

        @pl.when((kb == 4) & on_diag)
        def _():
            to_relay(chunks - 1).wait_recv()
            from_relay(chunks - 1).start()
            for index in range(chunks):
                side_group(index).start()

        @pl.when(kb == 5)
        def _():
            border_to(0, 0, to_side_id).wait_recv()
            pass_side(0).start()

        @pl.when(kb == 6)
        def _():
            pass_side(0).wait_recv()

            @pl.when(on_diag & (core == sent_part))
            def _():
                for index in range(chunks):
                    over_last(index).start()

        @pl.when((kb == 6) & on_diag)
        def _():
            side_group(0).wait_recv()
            pass_group(0).start()

        @pl.when((kb == 7) & on_diag)
        def _():
            pass_group(0).wait_recv()

            @pl.when(core != sent_part)
            def _():
                over_last(0).start()

            for index in range(1, chunks):
                side_group(index).wait_recv()
                pass_group(index).start()

    lane = lax.broadcasted_iota(jnp.int32, (BLOCK, order), 1)

    pair_lane = lax.broadcasted_iota(jnp.int32, (BLOCK, pair), 1)


    def block_step(kb, carry):
        pump_before(kb)
        start = pl.multiple_of(kb * BLOCK, BLOCK)
        here = pl.ds(start, BLOCK)

        def past_step(past, carry):
            there = pl.ds(pl.multiple_of(past * pair, pair), pair)
            known = pair_lane + past * pair < start
            top, mid, low = split_three(jnp.where(known, work[there, here].T, 0.0))
            work[here, there] = jnp.where(known, 0.0, work[here, there])
            first = jnp.dot(
                jnp.concatenate([top, mid, low], axis=0), rows_top[there, :],
                preferred_element_type=jnp.float32,
            )
            second = jnp.dot(
                jnp.concatenate([top, mid], axis=0), rows_mid[there, :],
                preferred_element_type=jnp.float32,
            )
            third = jnp.dot(top, rows_low[there, :], preferred_element_type=jnp.float32)
            small = (first[2 * BLOCK :] + third) + second[BLOCK:]
            change = first[:BLOCK] + ((first[BLOCK:pair] + second[:BLOCK]) + small)
            work[here, :] = work[here, :] - change
            return carry

        lax.fori_loop(0, (kb + 1) // 2, past_step, 0)

        @pl.when(kb % 2 == 1)
        def _():
            before = pl.ds(pl.multiple_of((kb - kb % 2) * BLOCK, BLOCK), BLOCK)
            for rows in (rows_top, rows_mid, rows_low):
                rows[before, here] = jnp.zeros((BLOCK, BLOCK), jnp.bfloat16)

        diag[...] = work[here, here]
        factor_diagonal(diag, upper, inv)
        pump_after(kb)
        work[here, here] = jnp.where(
            lax.broadcasted_iota(jnp.int32, (BLOCK, BLOCK), 0)
            == lax.broadcasted_iota(jnp.int32, (BLOCK, BLOCK), 1),
            1.0,
            0.0,
        )
        store_parts(parts, work[here, :])
        solved = six_pass(inv[...], [parts[index] for index in range(3)])
        low_part = jnp.where(lane < start + BLOCK, solved, 0.0)
        top, low = split_pair(low_part)
        inv_top[here, :] = top
        inv_low[here, :] = low
        work[here, :] = jnp.where(lane >= start + BLOCK, solved, 0.0)
        work[here, here] = upper[...]
        top, mid, low = split_three(solved)
        rows_top[here, :] = top
        rows_mid[here, :] = mid
        rows_low[here, :] = low
        return carry

    lax.fori_loop(0, count, block_step, 0)

    raw_top = rows_top
    raw_low = rows_mid
    own_top = rows_low
    own_rows = pl.ds(0, block)
    own_cols = pl.ds(0, cols_local)

    def solve_slots(left_top, left_low):
        for slot in range(slots):
            depth = (slot + 1) * piece_cols
            there = pl.ds(slot * piece_cols, piece_cols)
            result = dot_pair(
                (left_top[:block, :depth], left_low[:block, :depth]),
                (inv_top[there, :depth], inv_low[there, :depth]),
            )
            yield slot, there, result

    def solve_rows(part):
        def body(index, carry):
            source = pl.ds(pl.multiple_of(part * block + index * width, width), width)
            goal = pl.ds(pl.multiple_of(index * width, width), width)
            top, low = split_pair(rows_in[source, :])
            raw_top[goal, :] = top
            raw_low[goal, :] = low
            return carry

        lax.fori_loop(0, block // width, body, 0)
        for slot, there, result in solve_slots(raw_top, raw_low):
            top, low = split_pair(result)
            sol_top[:, there] = top
            sol_low[:, there] = low
            sol_full[:, there] = result
        border_out[spread(part, block), :] = sol_full[:, here_cols]

    reuse_sent = on_diag & (core == sent_part)
    reuse_own = on_diag & (core == own_part)

    def swap(index, thin):
        there = pl.ds(index * width if thin else 0, block - index * width if thin else block)
        return remote(
            sent.at[index, there], got.at[index, there],
            ssend.at[index], srecv.at[index], sibling_id,
        )

    def fill_place(index, later):
        return later * (later - 1) // 2 + index

    def share(index, later):
        return remote(
            got.at[index, pl.ds(later * width, width)], fill.at[fill_place(index, later)],
            tsend.at[index, later], trecv.at[index, later], to_far_id,
        )

    thin_send = core == sent_part
    thin_get = core == own_part

    def by_kind(thin, action):
        @pl.when(thin)
        def _():
            action(True)

        @pl.when(jnp.logical_not(thin))
        def _():
            action(False)

    def arrive(index):
        if index == 0:
            for part in range(chunks):
                swap_first(part).wait_recv()
        else:
            by_kind(thin_get, lambda thin: swap(index, thin).wait_recv())

        @pl.when(thin_get & off_diag)
        def _():
            for later in range(index + 1, chunks):
                share(index, later).start()

    def complete(index):
        for before in range(index):
            goal = pl.ds(before * width, width)

            @pl.when(thin_get & off_diag)
            def _(before=before, goal=goal):
                share(before, index).wait_recv()
                got[index, goal, :] = fill[fill_place(before, index)].T

            @pl.when(thin_get & on_diag)
            def _(before=before, goal=goal):
                got[index, goal, :] = got[before, pl.ds(index * width, width), :].T

    def swap_first(index):
        there = pl.ds(index * width, width)
        return remote(
            sent.at[0, there], got.at[0, there], hsend.at[index], hrecv.at[index], sibling_id
        )

    def make_cols(index):
        there = pl.ds(pl.multiple_of(index * width, width), width)

        @pl.when(off_diag)
        def _():
            where = cols_in.at[there, here_cols]
            for kind, target in ((1, to_side_id), (2, to_over_id), (3, to_over_id), (4, to_over_id)):
                remote(
                    where, where, xsend.at[kind, index], xrecv.at[kind, index], target
                ).wait_recv()

        @pl.when(reuse_own)
        def _():
            cols_in[there, :] = rows_in[group_rows(index), :]

        @pl.when(reuse_sent)
        def _():
            col_top[there, :] = sol_top[there, :]
            col_low[there, :] = sol_low[there, :]

        @pl.when(jnp.logical_not(reuse_sent))
        def _():
            top, low = split_pair(cols_in[there, :])
            for slot, place, result in solve_slots(top, low):
                top_part, low_part = split_pair(result)
                col_top[there, place] = top_part
                col_low[there, place] = low_part
                sol_full[there, place] = result

    def first_step(index, carry):
        there = pl.ds(pl.multiple_of(index * width, width), width)
        source = pl.ds(pl.multiple_of(sent_part * block + index * width, width), width)
        top, low = split_pair(rows_in[source, :])
        for slot, place, result in solve_slots(top, low):
            top_part, low_part = split_pair(result)
            sol_top[there, place] = top_part
            sol_low[there, place] = low_part
            sol_full[there, place] = result
        border_out[source, :] = sol_full[there, here_cols]

        @pl.when(index == 0)
        def _():
            make_cols(0)
            keep_sent(0).wait()

        change = dot_pair(
            (sol_top[there, :], sol_low[there, :]),
            (col_top[pl.ds(0, width), :], col_low[pl.ds(0, width), :]),
        )
        sent[0, there, :] = sent[0, there, :] - change
        for which in range(chunks):
            @pl.when(index == which)
            def _(which=which):
                swap_first(which).start()
        return carry

    lax.fori_loop(0, chunks, first_step, 0)

    @pl.when(on_diag)
    def _():
        for index in range(1, chunks):
            pass_group(index).wait_recv()

            @pl.when(core != sent_part)
            def _(index=index):
                over_last(index).start()

    @pl.when(off_diag)
    def _():
        for index in range(chunks):
            side_group(index).wait_recv()
            pass_group(index).start()

    def send_step(index, carry):
        there = pl.ds(pl.multiple_of(index * width, width), width)
        make_cols(index)
        pltpu.make_async_copy(
            update.at[pl.ds(0, block), pl.ds(0, width)], sent.at[index], osem.at[index]
        ).wait()
        change = dot_pair(
            (sol_top[...], sol_low[...]), (col_top[there, :], col_low[there, :])
        )
        sent[index] = sent[index] - change
        for which in range(1, chunks):
            @pl.when(index == which)
            def _(which=which):
                by_kind(thin_send, lambda thin: swap(which, thin).start())
        return carry

    lax.fori_loop(1, chunks, send_step, 0)

    piece = work[spread(col, piece_cols), spread(row, piece_rows)]
    pivot_out[...] = piece.T

    @pl.when(off_diag)
    def _():
        for index in range(chunks):
            pass_group(index).wait_recv()

    @pl.when(reuse_own)
    def _():
        sol_top[...] = col_top[...]
        sol_low[...] = col_low[...]
        border_out[spread(own_part, block), :] = sol_full[:, here_cols]

    @pl.when(jnp.logical_not(reuse_own))
    def _():
        solve_rows(own_part)

    keep_own.wait()

    def own_step(part, carry):
        there = spread(part, width)
        change = dot_pair(
            (sol_top[...], sol_low[...]), (col_top[there, :], col_low[there, :])
        )
        top, low = split_pair(own[:, there] - change)
        own_top[own_rows, there] = top
        own_low[:, there] = low
        return carry

    lax.fori_loop(0, cols_local // width, own_step, 0)

    keep_map.wait()
    keep_diag.wait()
    row_block = 2 * row + leaf_side
    third = half_rows // 3
    slack = half_rows - block

    def one_hot_rows(which, owner, position, base):
        def body(index, carry):
            here = pl.ds(pl.multiple_of(index * third, third), third)
            goal = maps[pl.ds(owner, 1), spread(position, block)] - base - index * third
            at = lax.broadcasted_iota(jnp.int32, (third, block), 0)
            hot[which, here, :] = jnp.where(at == goal, 1.0, 0.0).astype(jnp.bfloat16)
            return carry

        lax.fori_loop(0, half_rows // third, body, 0)

    def pick_t(left, right):
        return dot_t(left[0], right) + dot_t(left[1], right)

    def pick(left, right):
        return jnp.dot(left, right[0], preferred_element_type=jnp.float32) + jnp.dot(
            left, right[1], preferred_element_type=jnp.float32
        )

    def band(index):
        first = max(0, index * third - slack) // BLOCK * BLOCK
        return pl.ds(first, min(block, -(-(index + 1) * third // BLOCK) * BLOCK) - first)

    one_hot_rows(0, leaf, row_block, row_block * half_rows)
    one_hot_rows(1, leaf, col, col * parent_cols)

    for index in range(3):
        here = pl.ds(index * third, third)
        rows = band(index)
        wide = split_pair(pick(hot[0, here, rows], (own_top[rows, own_cols], own_low[rows, :])))
        raw_top[pl.ds(0, third), pl.ds(0, cols_local)] = wide[0]
        raw_low[pl.ds(0, third), pl.ds(0, cols_local)] = wide[1]
        for part in range(3):
            there = pl.ds(part * third, third)
            cols = band(part)
            result = pick_t(
                (raw_top[pl.ds(0, third), cols], raw_low[pl.ds(0, third), cols]),
                hot[1, there, cols],
            )
            if index == part:
                down = lax.broadcasted_iota(jnp.int32, (third, third), 0)
                across = lax.broadcasted_iota(jnp.int32, (third, third), 1)
                on_line = (down == across) & (row_block == col)
                result = result + jnp.where(on_line, diag_in[0:1, there], 0.0)
            parent_out[here, there] = result

    one_hot_rows(0, flip(leaf), row_block, row_block * half_rows)
    one_hot_rows(1, flip(leaf), col, col * parent_cols)

    for index in range(chunks):
        arrive(index)
        complete(index)
        low = index * width
        there = pl.ds(low, width + slack)
        arrived = split_pair(got[index])
        raw_top[own_rows, pl.ds(0, width)] = arrived[0]
        raw_low[own_rows, pl.ds(0, width)] = arrived[1]

        def got_step(part, carry, low=low, there=there):
            here = pl.ds(pl.multiple_of(part * third, third), third)
            some = pl.ds(0, width)
            wide = split_pair(
                pick(hot[0, here, :], (raw_top[own_rows, some], raw_low[own_rows, some]))
            )
            result = pick_t(wide, hot[1, there, pl.ds(low, width)])
            parent_out[here, there] = parent_out[here, there] + result
            return carry

        lax.fori_loop(0, 3, got_step, 0)

    @pl.when(below)
    def _():
        own_below().wait_send()

    @pl.when(off_diag)
    def _():
        for index in range(chunks):
            to_relay(index).wait_send()

    @pl.when(on_diag)
    def _():
        for index in range(chunks):
            from_relay(index).wait_send()
            over_first(index).wait_send()
            over_mate(index).wait_send()
            over_last(index).wait_send()

    border_to(0, 0, to_side_id).wait_send()
    pass_side(0).wait_send()
    for index in range(2):
        border_to(1, index, to_mate_id).wait_send()
    for chunk in range(pieces):
        @pl.when(piece_needed(row, col, chunk))
        def _(chunk=chunk):
            for index in (0, 1, 3):
                own_piece(index, chunk).wait_send()

            @pl.when(on_diag)
            def _():
                own_piece(2, chunk).wait_send()
    for index in range(chunks):
        swap_first(index).wait_send()
        side_group(index).wait_send()
        pass_group(index).wait_send()
    for index in range(1, chunks):
        by_kind(thin_send, lambda thin: swap(index, thin).wait_send())

    @pl.when(thin_get & off_diag)
    def _():
        for index in range(chunks):
            for later in range(index + 1, chunks):
                share(index, later).wait_send()


def store_kernel(*refs):
    copies = [
        pltpu.make_async_copy(refs[index], refs[3 + index], refs[6].at[index])
        for index in range(3)
    ]
    for copy in copies:
        copy.start()
    for copy in copies:
        copy.wait()


def whole_front(pivot, border, update, child_map, parent_diag, order):
    piece_rows, piece_cols = pivot.shape
    rows_local, cols_local = update.shape
    block = rows_local // 2
    width = piece_cols
    chunks = cols_local // width
    pieces = piece_rows // BLOCK
    half_rows = parent_diag.shape[1]
    parent_cols = half_rows
    vmem = pl.BlockSpec(memory_space=pltpu.VMEM)
    anywhere = pl.BlockSpec(memory_space=pl.ANY)
    dma = pltpu.SemaphoreType.DMA
    f32 = jnp.float32
    b16 = jnp.bfloat16
    results = pl.pallas_call(
        front_kernel,
        out_shape=(
            pltpu.VMEM((piece_rows, piece_cols), f32),
            pltpu.VMEM((rows_local, piece_cols), f32),
            pltpu.VMEM((half_rows, parent_cols), f32),
        ),
        in_specs=[pl.BlockSpec(memory_space=pltpu.HBM)] * 5,
        out_specs=(vmem, vmem, vmem),
        scratch_shapes=[
            pltpu.VMEM((order, order), f32),
            pltpu.VMEM((order, order), b16),
            pltpu.VMEM((order, order), b16),
            pltpu.VMEM((BLOCK, BLOCK), f32),
            pltpu.VMEM((BLOCK, BLOCK), f32),
            pltpu.VMEM((BLOCK, BLOCK), f32),
            pltpu.VMEM((3, 2 * BLOCK, order), b16),
            pltpu.VMEM((max(order, block), order), b16),
            pltpu.VMEM((max(order, block), order), b16),
            pltpu.VMEM((max(order, block), order), b16),
            pltpu.VMEM((block, order), b16),
            pltpu.VMEM((block, order), b16),
            pltpu.VMEM((block, order), f32),
            pltpu.VMEM((block, order), b16),
            pltpu.VMEM((block, order), b16),
            pltpu.VMEM((block, cols_local), b16),
            pltpu.VMEM((rows_local, order), f32),
            pltpu.VMEM((block, order), f32),
            pltpu.VMEM((block, piece_cols), f32),
            pltpu.VMEM((chunks, block, width), f32),
            pltpu.VMEM((block, cols_local), f32),
            pltpu.VMEM((chunks, block, width), f32),
            pltpu.VMEM((chunks * (chunks - 1) // 2, width, width), f32),
            pltpu.VMEM(child_map.shape, jnp.int32),
            pltpu.VMEM(parent_diag.shape, f32),
            pltpu.VMEM((2, half_rows, block), b16),
            dma((5,)), dma((4, pieces)), dma((4, pieces)), dma((3, pieces)), dma((3, pieces)),
            dma((3, 2)), dma((3, 2)), dma((5, chunks)), dma((5, chunks)),
            dma((chunks,)), dma((chunks,)), dma((chunks,)),
            dma((chunks, chunks)), dma((chunks, chunks)),
            dma((chunks,)), dma((chunks,)), dma((2, chunks)), dma((2, chunks)),
        ],
        compiler_params=pltpu.CompilerParams(
            vmem_limit_bytes=56 * 2**20, collective_id=0, has_side_effects=True
        ),
        name="whole_front",
    )(pivot, border, update, child_map, parent_diag)
    return pl.pallas_call(
        store_kernel,
        out_shape=tuple(jax.ShapeDtypeStruct(result.shape, f32) for result in results),
        in_specs=[vmem] * 3,
        out_specs=(pl.BlockSpec(memory_space=pltpu.HBM),) * 3,
        scratch_shapes=[dma((3,))],
        compiler_params=pltpu.CompilerParams(vmem_limit_bytes=2**20),
        name="store_results",
    )(*results)


def high_dot_t(left, right):
    return lax.dot_general(
        left, right, (((1,), (1,)), ((), ())), precision=HIGH, preferred_element_type=jnp.float32
    )


def split_two(value):
    top = lax.reduce_precision(value, 8, 7)
    return top.astype(jnp.bfloat16), (value - top).astype(jnp.bfloat16)


def one_hot(targets, size):
    return (jnp.arange(size, dtype=jnp.int32)[:, None] == targets[None, :]).astype(jnp.bfloat16)


def pick_dot(left, right, dims):
    return lax.dot_general(left, right, (dims, ((), ())), preferred_element_type=jnp.float32)


def place_blocks(blocks, rows_to, cols_to, out_rows, out_cols):
    col_hot = one_hot(cols_to, out_cols)
    first = 0
    placed = None
    for block in blocks:
        count = block.shape[0]
        row_hot = one_hot(rows_to[first : first + count], out_rows)
        first += count
        top, rest = split_two(block)
        wide = pick_dot(top, col_hot, ((1,), (1,))) + pick_dot(rest, col_hot, ((1,), (1,)))
        top, rest = split_two(wide)
        part = pick_dot(row_hot, top, ((1,), (0,))) + pick_dot(row_hot, rest, ((1,), (0,)))
        placed = part if placed is None else placed + part
    return placed


def column_border(bord, full_rows, nrow, ncol, cols_local, row_index, col_index):
    rows_local, width = bord.shape
    if nrow == 2 and rows_local % cols_local == 0:
        per_row = rows_local // cols_local
        mine = lax.dynamic_slice_in_dim(full_rows, (col_index % per_row) * cols_local, cols_local, 0)
        received = jnp.zeros((cols_local, full_rows.shape[1]), bord.dtype)
        for shift in range(ncol):
            pairs = []
            for c in range(ncol):
                home = c // per_row
                pairs.append((home * ncol + (c + shift) % ncol, (1 - home) * ncol + c))
            target = (col_index - shift + ncol) % ncol
            part = lax.dynamic_slice_in_dim(bord, (target % per_row) * cols_local, cols_local, 0)
            moved = lax.ppermute(part, ("row", "col"), pairs)
            place = (col_index + shift) % ncol * width
            received = lax.dynamic_update_slice_in_dim(received, moved, place, 1)
        return jnp.where(row_index == col_index // per_row, mine, received)
    whole = lax.all_gather(full_rows, "row", axis=0, tiled=True)
    return lax.dynamic_slice_in_dim(whole, col_index * cols_local, cols_local, 0)


def fits(nrow, ncol, pivot, border, update, child_map, parent_diag):
    rows, cols = update.shape
    half_rows = parent_diag.shape[1]
    return (
        nrow == 2
        and ncol == 4
        and pivot.shape[0] == 2 * pivot.shape[1]
        and rows == 2 * cols
        and border.shape == (rows, pivot.shape[1])
        and child_map.shape[1] == nrow * rows
        and pivot.shape[1] % (2 * BLOCK) == 0
        and cols % pivot.shape[1] == 0
        and half_rows % (3 * BLOCK) == 0
        and half_rows > cols
    )


def on_device(pivot, border, update, child_map, parent_diag):
    nrow = lax.axis_size("row")
    ncol = lax.axis_size("col")
    row_index = lax.axis_index("row")
    col_index = lax.axis_index("col")
    leaf_index = lax.axis_index("leaf")
    piece = pivot[0]
    piece_rows, piece_cols = piece.shape
    if fits(nrow, ncol, piece, border[0], update[0], child_map, parent_diag):
        order = nrow * piece_rows
        outs = whole_front(piece, border[0], update[0], child_map, parent_diag, order)
        return tuple(out[None] for out in outs)
    stacked = lax.all_gather(piece[None], ("row", "col"), axis=0, tiled=True)
    stacked, bord = lax.optimization_barrier((stacked, border[0]))
    upper, inverse = factor(stacked, nrow * piece_rows)
    pivot_out = lax.dynamic_slice(
        upper, (col_index * piece_cols, row_index * piece_rows), (piece_cols, piece_rows)
    ).T

    rows_local = bord.shape[0]
    trailing = update[0]
    cols_local = trailing.shape[1]
    full_rows = lax.all_gather(bord, "col", axis=1, tiled=True)
    col_rows = column_border(bord, full_rows, nrow, ncol, cols_local, row_index, col_index)
    factor_cols = high_dot_t(col_rows, inverse)

    half_rows = parent_diag.shape[1]
    block_rows = 2 * half_rows
    parent_cols = block_rows * nrow // ncol
    side = leaf_index % 2
    partner = leaf_index + 1 - 2 * side
    total_cols = child_map.shape[1]
    own_map = lax.dynamic_slice(child_map, (leaf_index, 0), (1, total_cols))[0]
    partner_map = lax.dynamic_slice(child_map, (partner, 0), (1, total_cols))[0]
    swap = [(source, source ^ 1) for source in range(lax.axis_size("leaf"))]

    map_block = total_cols // max(nrow, ncol)
    halves = rows_local % (2 * map_block) == 0
    if halves:
        kept = rows_local // 2
        own_start = side * kept
        sent_start = (1 - side) * kept

        def schur_rows(start, size):
            rows = lax.dynamic_slice_in_dim(full_rows, start, size, 0)
            below = high_dot_t(rows, inverse)
            part = lax.dynamic_slice_in_dim(trailing, start, size, 0)
            return below, part - high_dot_t(below, factor_cols)

        sent_parts = []
        sibling = []
        chunk = kept // CHUNKS
        for index in range(CHUNKS):
            below, sent = schur_rows(sent_start + index * chunk, chunk)
            sent_parts.append(below)
            sibling.append(lax.ppermute(sent, "leaf", swap))
        sent_below = jnp.concatenate(sent_parts, axis=0)
        own_below, own = schur_rows(own_start, kept)
        own_slice = lax.dynamic_slice_in_dim(own_below, col_index * piece_cols, piece_cols, 1)
        sent_slice = lax.dynamic_slice_in_dim(sent_below, col_index * piece_cols, piece_cols, 1)
        border_out = jnp.where(
            side == 0,
            jnp.concatenate([own_slice, sent_slice], axis=0),
            jnp.concatenate([sent_slice, own_slice], axis=0),
        )
    else:
        kept = rows_local
        own_start = 0
        factor_rows = high_dot_t(full_rows, inverse)
        own = trailing - high_dot_t(factor_rows, factor_cols)
        sibling = [lax.ppermute(own, "leaf", swap)]
        border_out = lax.dynamic_slice_in_dim(factor_rows, col_index * piece_cols, piece_cols, 1)

    def my_half(blocks, mapping):
        rows_to = (
            lax.dynamic_slice_in_dim(mapping, row_index * rows_local + own_start, kept)
            - row_index * block_rows
            - side * half_rows
        )
        cols_to = (
            lax.dynamic_slice_in_dim(mapping, col_index * cols_local, cols_local)
            - col_index * parent_cols
        )
        return place_blocks(blocks, rows_to, cols_to, half_rows, parent_cols)

    global_rows = row_index * block_rows + side * half_rows + jnp.arange(half_rows, dtype=jnp.int32)
    global_cols = col_index * parent_cols + jnp.arange(parent_cols, dtype=jnp.int32)
    diagonal = jnp.where(global_rows[:, None] == global_cols[None, :], parent_diag[0][:, None], 0.0)
    parent_out = my_half([own], own_map) + diagonal + my_half(sibling, partner_map)
    return (pivot_out[None], border_out[None], parent_out[None])


def solution(mesh):
    placed = (
        P("leaf", "row", "col"),
        P("leaf", "row", "col"),
        P("leaf", "row", "col"),
        P(),
        P("leaf", "row"),
    )
    return jax.shard_map(
        on_device,
        mesh=mesh,
        in_specs=placed,
        out_specs=(P("leaf", "row", "col"), P("leaf", "row", "col"), P("leaf", "row", "col")),
        check_vma=False,
    )
```

```python
import jax
import jax.numpy as jnp
from jax import lax
from jax.experimental import pallas as pl
from jax.experimental.pallas import tpu as pltpu
from jax.sharding import PartitionSpec as P

BLOCK = 128
CHUNKS = 2
PANEL = 8
HIGH = lax.Precision.HIGH


def exact_dot(left, right):
    return jnp.dot(left, right, precision=lax.Precision.HIGHEST, preferred_element_type=jnp.float32)


def factor_small(entry):
    work = {key: value for key, value in entry.items()}
    lower = {}
    inverse = {}
    for k in range(PANEL):
        scale = lax.rsqrt(work[k, k])
        for i in range(k + 1, PANEL):
            lower[i, k] = work[i, k] * scale
        for j in range(k + 1, PANEL):
            for i in range(j, PANEL):
                work[i, j] = work[i, j] - lower[i, k] * lower[j, k]
        inverse[k, k] = scale
        for j in range(k):
            total = lower[k, j] * inverse[j, j]
            for m in range(j + 1, k):
                total = total + lower[k, m] * inverse[m, j]
            inverse[k, j] = -(total * scale)
    return inverse


def factor_block(diag, upper, inv):
    lane8 = lax.broadcasted_iota(jnp.int32, (PANEL, BLOCK), 1)
    lane_all = lax.broadcasted_iota(jnp.int32, (BLOCK, BLOCK), 1)

    def panel_step(p, carry):
        base = p * PANEL
        start = pl.multiple_of(base, PANEL)
        rows = diag[pl.ds(start, PANEL), :]
        full = diag[...]
        entry = {}
        for b in range(PANEL):
            index = jnp.zeros((PANEL, BLOCK), jnp.int32) + (base + b)
            col = jnp.take_along_axis(rows, index, axis=1, mode="promise_in_bounds")
            for a in range(b, PANEL):
                entry[a, b] = jnp.broadcast_to(col[a : a + 1, :], (PANEL, BLOCK))
        inverse = factor_small(entry)
        inside = (lane8 >= base) & (lane8 < base + PANEL)
        plain = []
        augmented = []
        for k in range(PANEL):
            row = jnp.broadcast_to(rows[k : k + 1, :], (PANEL, BLOCK))
            plain.append(row)
            augmented.append(jnp.where(inside, (lane8 == base + k).astype(jnp.float32), row))
        solved = []
        for a in range(PANEL):
            up = inverse[a, 0] * plain[0]
            au = inverse[a, 0] * augmented[0]
            for k in range(1, a + 1):
                up = up + inverse[a, k] * plain[k]
                au = au + inverse[a, k] * augmented[k]
            solved.append(au)
            keep = lane8 >= base + a
            upper[pl.ds(start + a, 1), :] = jnp.where(keep, up, 0.0)[0:1, :]
            inv[pl.ds(start + a, 1), :] = jnp.where(lane8 <= base + a, au, 0.0)[0:1, :]
        inside_all = (lane_all >= base) & (lane_all < base + PANEL)
        trailing = jnp.where(inside_all, 0.0, full)
        for m in range(PANEL):
            gain = inverse[m, m] * solved[m]
            for a in range(m + 1, PANEL):
                gain = gain + inverse[a, m] * solved[a]
            index = jnp.zeros((BLOCK, BLOCK), jnp.int32) + (base + m)
            col = jnp.take_along_axis(full, index, axis=1, mode="promise_in_bounds")
            trailing = trailing - col * jnp.broadcast_to(gain[0:1, :], (BLOCK, BLOCK))
        diag[...] = trailing
        return carry

    lax.fori_loop(0, BLOCK // PANEL, panel_step, 0)


def split_three(value):
    top = value.astype(jnp.bfloat16)
    rest = value - top.astype(jnp.float32)
    mid = rest.astype(jnp.bfloat16)
    return top, mid, (rest - mid.astype(jnp.float32)).astype(jnp.bfloat16)


def factor_steps(work, diag, upper, inv, panel, parts, finish, pump=None):
    order = work.shape[0]
    count = order // BLOCK

    def block_step(kb, carry):
        if pump is not None:
            pump(kb)
        start = pl.multiple_of(kb * BLOCK, BLOCK)
        here = pl.ds(start, BLOCK)
        diag[...] = work[here, here]
        factor_block(diag, upper, inv)
        work[here, here] = jnp.where(
            lax.broadcasted_iota(jnp.int32, (BLOCK, BLOCK), 0)
            == lax.broadcasted_iota(jnp.int32, (BLOCK, BLOCK), 1),
            1.0,
            0.0,
        )
        panel[...] = exact_dot(inv[...], work[here, :])
        solved = panel[...]
        finish(start, here, solved)

        top, mid, low = split_three(solved)
        parts[0, :BLOCK, :] = top
        parts[0, BLOCK:, :] = top
        parts[1, :BLOCK, :] = mid
        parts[1, BLOCK:, :] = mid
        parts[2, :BLOCK, :] = low
        parts[2, BLOCK:, :] = top

        def row_step(ib, carry):
            there = pl.ds(pl.multiple_of(ib * BLOCK, BLOCK), BLOCK)
            top, mid, low = split_three(panel[:, there].T)
            both = jnp.concatenate([top, mid], axis=1)
            ends = jnp.concatenate([top, low], axis=1)
            change = jnp.dot(ends, parts[2], preferred_element_type=jnp.float32)
            change = change + jnp.dot(both, parts[1], preferred_element_type=jnp.float32)
            change = change + jnp.dot(both, parts[0], preferred_element_type=jnp.float32)
            work[there, here] = jnp.zeros((BLOCK, BLOCK), jnp.float32)
            work[there, :] = work[there, :] - change
            return carry

        lax.fori_loop(kb + 1, count, row_step, 0)
        return carry

    lax.fori_loop(0, count, block_step, 0)


def factor_kernel(pivot, upper_out, inverse_out, work, diag, upper, inv, panel, parts):
    order = work.shape[0]
    lane = lax.broadcasted_iota(jnp.int32, (BLOCK, order), 1)
    pieces, piece_rows, piece_cols = pivot.shape
    across = order // piece_cols
    for index in range(pieces):
        first_row = index // across * piece_rows
        first_col = index % across * piece_cols
        if first_row < first_col + piece_cols:
            work[pl.ds(first_row, piece_rows), pl.ds(first_col, piece_cols)] = pivot[index]
        else:
            work[pl.ds(first_row, piece_rows), pl.ds(first_col, piece_cols)] = jnp.zeros(
                (piece_rows, piece_cols), jnp.float32
            )

    def finish(start, here, solved):
        inverse_out[here, :] = jnp.where(lane < start + BLOCK, solved, 0.0)
        upper_out[here, :] = jnp.where(lane >= start + BLOCK, solved, 0.0)
        upper_out[here, here] = upper[...]

    factor_steps(work, diag, upper, inv, panel, parts, finish)


def factor(pivot, order):
    spec = pl.BlockSpec(memory_space=pltpu.VMEM)
    shape = jax.ShapeDtypeStruct((order, order), jnp.float32)
    return pl.pallas_call(
        factor_kernel,
        out_shape=(shape, shape),
        in_specs=[spec],
        out_specs=(spec, spec),
        scratch_shapes=[
            pltpu.VMEM((order, order), jnp.float32),
            pltpu.VMEM((BLOCK, BLOCK), jnp.float32),
            pltpu.VMEM((BLOCK, BLOCK), jnp.float32),
            pltpu.VMEM((BLOCK, BLOCK), jnp.float32),
            pltpu.VMEM((BLOCK, order), jnp.float32),
            pltpu.VMEM((3, 2 * BLOCK, order), jnp.bfloat16),
        ],
        compiler_params=pltpu.CompilerParams(vmem_limit_bytes=40 * 2**20),
        cost_estimate=pl.CostEstimate(
            flops=60 * order**3, bytes_accessed=12 * order * order, transcendentals=order
        ),
        name="factor",
    )(pivot)


def flip(value):
    return value + 1 - 2 * (value % 2)


def remote(src, dst, send, recv, target):
    return pltpu.make_async_remote_copy(
        src_ref=src,
        dst_ref=dst,
        send_sem=send,
        recv_sem=recv,
        device_id=target,
        device_id_type=pl.DeviceIdType.MESH,
    )


def lane_column(rows, place):
    index = jnp.full(rows.shape, place, jnp.int32)
    return jnp.take_along_axis(rows, index, axis=1, mode="promise_in_bounds")


def factor_diagonal(diag, upper, inv):
    lane = lax.broadcasted_iota(jnp.int32, (PANEL, BLOCK), 1)
    count = BLOCK // PANEL
    rows = [diag[pl.ds(index * PANEL, PANEL), :] for index in range(count)]
    for step in range(count):
        base = step * PANEL
        entry = {}
        for b in range(PANEL):
            column = lane_column(rows[step], base + b)
            for a in range(b, PANEL):
                entry[a, b] = jnp.broadcast_to(column[a : a + 1, :], (PANEL, BLOCK))
        inverse = factor_small(entry)
        inside = (lane >= base) & (lane < base + PANEL)
        plain = []
        augmented = []
        for k in range(PANEL):
            line = jnp.broadcast_to(rows[step][k : k + 1, :], (PANEL, BLOCK))
            plain.append(line)
            augmented.append(jnp.where(inside, (lane == base + k).astype(jnp.float32), line))
        solved = []
        for a in range(PANEL):
            up = inverse[a, 0] * plain[0]
            au = inverse[a, 0] * augmented[0]
            for k in range(1, a + 1):
                up = up + inverse[a, k] * plain[k]
                au = au + inverse[a, k] * augmented[k]
            solved.append(au)
            upper[pl.ds(base + a, 1), :] = jnp.where(lane >= base + a, up, 0.0)[0:1, :]
            inv[pl.ds(base + a, 1), :] = jnp.where(lane <= base + a, au, 0.0)[0:1, :]
        if step + 1 == count:
            break
        gains = []
        for m in range(PANEL):
            gain = inverse[m, m] * solved[m]
            for a in range(m + 1, PANEL):
                gain = gain + inverse[a, m] * solved[a]
            gains.append(gain)
        for later in range(step + 1, count):
            value = jnp.where(inside, 0.0, rows[later])
            for m in range(PANEL):
                value = value - lane_column(rows[later], base + m) * gains[m]
            rows[later] = value


def six_pass(left, parts):
    top, mid, low = split_three(left)
    both = jnp.concatenate([top, mid], axis=1)
    ends = jnp.concatenate([top, low], axis=1)
    change = jnp.dot(ends, parts[2], preferred_element_type=jnp.float32)
    change = change + jnp.dot(both, parts[1], preferred_element_type=jnp.float32)
    return change + jnp.dot(both, parts[0], preferred_element_type=jnp.float32)


def store_parts(parts, value):
    top, mid, low = split_three(value)
    parts[0, :BLOCK, :] = top
    parts[0, BLOCK:, :] = top
    parts[1, :BLOCK, :] = mid
    parts[1, BLOCK:, :] = mid
    parts[2, :BLOCK, :] = low
    parts[2, BLOCK:, :] = top


def split_pair(value):
    top = value.astype(jnp.bfloat16)
    return top, (value - top.astype(jnp.float32)).astype(jnp.bfloat16)


def dot_t(left, right):
    return lax.dot_general(
        left, right, (((1,), (1,)), ((), ())), preferred_element_type=jnp.float32
    )


def dot_pair(left, right):
    return dot_t(left[0], right[0]) + (dot_t(left[0], right[1]) + dot_t(left[1], right[0]))


def front_kernel(
    pivot, border, update, child_map, parent_diag, pivot_out, border_out, parent_out,
    work, inv_top, inv_low, diag, upper, inv, parts, rows_top, rows_mid, rows_low,
    sol_top, sol_low, sol_full, col_top, col_low, own_low,
    rows_in, cols_in, relay, sent, own, got, fill, maps, diag_in, hot,
    local_sem, psend, precv, fsend, frecv, bsend, brecv, xsend, xrecv, ssend, srecv, osem,
    tsend, trecv, hsend, hrecv, gsend, grecv,
):
    leaf = lax.axis_index("leaf")
    row = lax.axis_index("row")
    col = lax.axis_index("col")
    core = col % 2
    cross = (col + 2) % 4
    mate = flip(col)
    mate_cross = (mate + 2) % 4
    leaf_side = leaf % 2
    on_diag = row == col // 2
    off_diag = jnp.logical_not(on_diag)
    to_mate_id = (leaf, row, mate)
    to_side_id = (leaf, row, cross)
    to_over_id = (leaf, 1 - row, col)
    to_far_id = (leaf, 1 - row, cross)
    sibling_id = (flip(leaf), row, col)

    piece_rows, piece_cols = pivot.shape
    order = work.shape[0]
    rows_local, cols_local = update.shape
    block = rows_local // 2
    chunks, _, width = sent.shape
    pieces = piece_rows // BLOCK
    half_rows = parent_out.shape[0]
    parent_cols = parent_out.shape[1]
    slots = order // piece_cols
    count = order // BLOCK

    barrier = pltpu.get_barrier_semaphore()
    for target in (to_mate_id, to_side_id, to_over_id, to_far_id, sibling_id):
        pl.semaphore_signal(
            barrier, inc=1, device_id=target, device_id_type=pl.DeviceIdType.MESH
        )

    def spread(value, size):
        return pl.ds(pl.multiple_of(value * size, size), size)

    sent_part = 1 - leaf_side
    own_part = leaf_side
    here_rows = spread(row, piece_rows)
    here_cols = spread(col, piece_cols)
    keep_pivot = pltpu.make_async_copy(pivot, work.at[here_rows, here_cols], local_sem.at[0])
    keep_border = pltpu.make_async_copy(border, rows_in.at[:, here_cols], local_sem.at[1])
    keep_map = pltpu.make_async_copy(child_map, maps, local_sem.at[2])
    keep_diag = pltpu.make_async_copy(parent_diag, diag_in, local_sem.at[3])
    keep_own = pltpu.make_async_copy(update.at[spread(own_part, block)], own, local_sem.at[4])

    def keep_sent(index):
        return pltpu.make_async_copy(
            update.at[spread(sent_part, block), pl.ds(index * width, width)],
            sent.at[index],
            osem.at[index],
        )

    keep_pivot.start()
    keep_border.start()
    keep_map.start()
    keep_diag.start()
    pair = 2 * BLOCK

    def clear_step(index, carry):
        there = pl.ds(pl.multiple_of(index * BLOCK, BLOCK), BLOCK)
        for rows in (rows_top, rows_mid, rows_low):
            rows[there, :] = jnp.zeros((BLOCK, order), jnp.bfloat16)
        return carry

    lax.fori_loop(0, count, clear_step, 0)
    pl.semaphore_wait(barrier, 5)

    targets = (to_over_id, to_side_id, to_far_id, to_mate_id)
    remote_slots = ((1 - row, col), (row, cross), (1 - row, cross))
    mate_slots = ((1 - row, mate), (row, mate_cross), (1 - row, mate_cross))

    def piece_needed(source_row, source_col, chunk):
        return (source_col + 1) * (piece_cols // BLOCK) > source_row * pieces + chunk

    def own_piece(index, chunk):
        there = pl.ds(pl.multiple_of(row * piece_rows + chunk * BLOCK, BLOCK), BLOCK)
        return remote(
            pivot.at[pl.ds(chunk * BLOCK, BLOCK)], work.at[there, here_cols],
            psend.at[index, chunk], precv.at[index, chunk], targets[index],
        )

    def pass_piece(index, chunk, source_row, source_col):
        there = pl.ds(pl.multiple_of(source_row * piece_rows + chunk * BLOCK, BLOCK), BLOCK)
        where = work.at[there, spread(source_col, piece_cols)]
        return remote(
            where, where, fsend.at[index, chunk], frecv.at[index, chunk], to_mate_id
        )

    below = row > col // 2

    def own_below():
        where = work.at[here_rows, here_cols]
        return remote(pivot, where, psend.at[3, 0], precv.at[3, 0], to_mate_id)

    @pl.when(below)
    def _():
        own_below().start()

    for chunk in range(pieces):
        @pl.when(piece_needed(row, col, chunk))
        def _(chunk=chunk):
            for index in (0, 1, 3):
                own_piece(index, chunk).start()

            @pl.when(on_diag & (row == 0))
            def _():
                own_piece(2, chunk).start()

    def part_of(index):
        return sent_part if index == 0 else own_part

    def border_to(kind, index, target):
        there = spread(part_of(index), block)
        return remote(
            border.at[there], rows_in.at[there, here_cols],
            bsend.at[kind, index], brecv.at[kind, index], target,
        )

    def pass_side(index):
        where = rows_in.at[spread(part_of(index), block), spread(cross, piece_cols)]
        return remote(where, where, bsend.at[2, index], brecv.at[2, index], to_mate_id)

    core_rows = spread(core, block)

    def group_rows(index):
        return pl.ds(pl.multiple_of(core * block + index * width, width), width)

    def to_relay(index):
        return remote(
            border.at[group_rows(index)], relay.at[pl.ds(index * width, width)],
            xsend.at[0, index], xrecv.at[0, index], to_over_id,
        )

    def from_relay(index):
        there = pl.ds(index * width, width)
        return remote(
            relay.at[there], cols_in.at[there, here_cols],
            xsend.at[1, index], xrecv.at[1, index], to_side_id,
        )

    def over_first(index):
        return remote(
            border.at[group_rows(index)], cols_in.at[pl.ds(index * width, width), here_cols],
            xsend.at[2, index], xrecv.at[2, index], to_over_id,
        )

    def over_slot(kind, which, index):
        where = spread(which, piece_cols)
        return remote(
            rows_in.at[group_rows(index), where], cols_in.at[pl.ds(index * width, width), where],
            xsend.at[kind, index], xrecv.at[kind, index], to_over_id,
        )

    def over_mate(index):
        return over_slot(3, mate, index)

    def over_last(index):
        return over_slot(4, mate_cross, index)

    def own_group(kind, index, which, target):
        there = pl.ds(pl.multiple_of(own_part * block + index * width, width), width)
        where = rows_in.at[there, spread(which, piece_cols)]
        source = border.at[there] if kind == 0 else where
        return remote(source, where, gsend.at[kind, index], grecv.at[kind, index], target)

    def side_group(index):
        return own_group(0, index, col, to_side_id)

    def pass_group(index):
        return own_group(1, index, cross, to_mate_id)

    @pl.when(jnp.logical_not(below))
    def _():
        border_to(0, 0, to_side_id).start()

    for index in range(2):
        border_to(1, index, to_mate_id).start()

    @pl.when(on_diag)
    def _():
        over_first(0).start()

    for chunk in range(pieces):
        @pl.when(on_diag & (row == 1) & piece_needed(row, col, chunk))
        def _(chunk=chunk):
            own_piece(2, chunk).start()

    @pl.when(on_diag)
    def _():
        for index in range(1, chunks):
            over_first(index).start()

    @pl.when(off_diag)
    def _():
        for index in range(chunks):
            to_relay(index).start()

    @pl.when(off_diag & jnp.logical_not(below))
    def _():
        for index in range(chunks):
            side_group(index).start()

    def forward_row(source_row, chunk, pick=lambda which: True):
        for index, (from_row, from_col) in enumerate(remote_slots):
            chosen = (from_row == source_row) & pick(from_col)
            if index == 2:
                chosen = chosen & (from_row == from_col // 2)

            @pl.when(chosen & piece_needed(from_row, from_col, chunk))
            def _(index=index, from_row=from_row, from_col=from_col):
                own_piece(index, chunk).wait_recv()
                pass_piece(index, chunk, from_row, from_col).start()

    def collect_row(source_row, chunk, pick=lambda which: True):
        @pl.when((row == source_row) & pick(mate) & piece_needed(row, mate, chunk))
        def _():
            own_piece(3, chunk).wait_recv()
        for index, (from_row, from_col) in enumerate(mate_slots):
            chosen = (from_row == source_row) & pick(from_col)
            if index == 2:
                chosen = chosen & (from_row == from_col // 2)

            @pl.when(chosen & piece_needed(from_row, from_col, chunk))
            def _(index=index):
                pass_piece(index, chunk, row, col).wait_recv()
        for index, (from_row, from_col) in enumerate(remote_slots):
            chosen = (from_row == source_row) & pick(from_col)
            if index == 2:
                chosen = chosen & (from_row == from_col // 2)

            @pl.when(chosen & piece_needed(from_row, from_col, chunk))
            def _(index=index):
                pass_piece(index, chunk, row, col).wait_send()

    def is_first(which):
        return which == 0

    def is_later(which):
        return which > 0

    def pump_before(kb):
        @pl.when(kb == 0)
        def _():
            keep_pivot.wait()

            @pl.when(below)
            def _():
                own_below().wait_recv()
                for which in range(2):
                    value = work[pl.ds(piece_rows, piece_rows), pl.ds(which * piece_cols, piece_cols)]
                    work[pl.ds(which * piece_cols, piece_cols), pl.ds(piece_rows, piece_rows)] = value.T

            forward_row(0, 0, is_first)
            collect_row(0, 0, is_first)
        for step in range(1, count):
            @pl.when(kb == step)
            def _(step=step):
                collect_row(step // pieces, step % pieces)

    def pump_after(kb):
        @pl.when(kb == 0)
        def _():
            forward_row(0, 0, is_later)
            collect_row(0, 0, is_later)
        for step in range(count - 1):
            @pl.when(kb == step)
            def _(step=step):
                forward_row((step + 1) // pieces, (step + 1) % pieces)

        @pl.when(kb == 0)
        def _():
            keep_own.start()
            for index in range(chunks):
                keep_sent(index).start()

        @pl.when(kb == 1)
        def _():
            keep_border.wait()
            for index in range(2):
                border_to(1, index, to_mate_id).wait_recv()

            @pl.when(on_diag)
            def _():
                for index in range(chunks):
                    over_mate(index).start()

        @pl.when((kb == 1) & below)
        def _():
            border_to(0, 0, to_side_id).start()
            for index in range(chunks):
                side_group(index).start()

        @pl.when((kb == 3) & on_diag)
        def _():
            for index in range(chunks - 1):
                to_relay(index).wait_recv()
                from_relay(index).start()

        @pl.when((kb == 4) & on_diag)
        def _():
            to_relay(chunks - 1).wait_recv()
            from_relay(chunks - 1).start()
            for index in range(chunks):
                side_group(index).start()

        @pl.when(kb == 5)
        def _():
            border_to(0, 0, to_side_id).wait_recv()
            pass_side(0).start()

        @pl.when(kb == 6)
        def _():
            pass_side(0).wait_recv()

            @pl.when(on_diag & (core == sent_part))
            def _():
                for index in range(chunks):
                    over_last(index).start()

        @pl.when((kb == 6) & on_diag)
        def _():
            side_group(0).wait_recv()
            pass_group(0).start()

        @pl.when((kb == 7) & on_diag)
        def _():
            pass_group(0).wait_recv()

            @pl.when(core != sent_part)
            def _():
                over_last(0).start()

            for index in range(1, chunks):
                side_group(index).wait_recv()
                pass_group(index).start()

    lane = lax.broadcasted_iota(jnp.int32, (BLOCK, order), 1)

    pair_lane = lax.broadcasted_iota(jnp.int32, (BLOCK, pair), 1)


    def block_step(kb, carry):
        pump_before(kb)
        start = pl.multiple_of(kb * BLOCK, BLOCK)
        here = pl.ds(start, BLOCK)

        def past_step(past, carry):
            there = pl.ds(pl.multiple_of(past * pair, pair), pair)
            known = pair_lane + past * pair < start
            top, mid, low = split_three(jnp.where(known, work[there, here].T, 0.0))
            work[here, there] = jnp.where(known, 0.0, work[here, there])
            first = jnp.dot(
                jnp.concatenate([top, mid, low], axis=0), rows_top[there, :],
                preferred_element_type=jnp.float32,
            )
            second = jnp.dot(
                jnp.concatenate([top, mid], axis=0), rows_mid[there, :],
                preferred_element_type=jnp.float32,
            )
            third = jnp.dot(top, rows_low[there, :], preferred_element_type=jnp.float32)
            small = (first[2 * BLOCK :] + third) + second[BLOCK:]
            change = first[:BLOCK] + ((first[BLOCK:pair] + second[:BLOCK]) + small)
            work[here, :] = work[here, :] - change
            return carry

        lax.fori_loop(0, (kb + 1) // 2, past_step, 0)

        @pl.when(kb % 2 == 1)
        def _():
            before = pl.ds(pl.multiple_of((kb - kb % 2) * BLOCK, BLOCK), BLOCK)
            for rows in (rows_top, rows_mid, rows_low):
                rows[before, here] = jnp.zeros((BLOCK, BLOCK), jnp.bfloat16)

        diag[...] = work[here, here]
        factor_diagonal(diag, upper, inv)
        pump_after(kb)
        work[here, here] = jnp.where(
            lax.broadcasted_iota(jnp.int32, (BLOCK, BLOCK), 0)
            == lax.broadcasted_iota(jnp.int32, (BLOCK, BLOCK), 1),
            1.0,
            0.0,
        )
        store_parts(parts, work[here, :])
        solved = six_pass(inv[...], [parts[index] for index in range(3)])
        low_part = jnp.where(lane < start + BLOCK, solved, 0.0)
        top, low = split_pair(low_part)
        inv_top[here, :] = top
        inv_low[here, :] = low
        work[here, :] = jnp.where(lane >= start + BLOCK, solved, 0.0)
        work[here, here] = upper[...]
        top, mid, low = split_three(solved)
        rows_top[here, :] = top
        rows_mid[here, :] = mid
        rows_low[here, :] = low
        return carry

    lax.fori_loop(0, count, block_step, 0)

    raw_top = rows_top
    raw_low = rows_mid
    own_top = rows_low
    own_rows = pl.ds(0, block)
    own_cols = pl.ds(0, cols_local)

    def solve_slots(left_top, left_low):
        for slot in range(slots):
            depth = (slot + 1) * piece_cols
            there = pl.ds(slot * piece_cols, piece_cols)
            result = dot_pair(
                (left_top[:block, :depth], left_low[:block, :depth]),
                (inv_top[there, :depth], inv_low[there, :depth]),
            )
            yield slot, there, result

    def solve_rows(part):
        def body(index, carry):
            source = pl.ds(pl.multiple_of(part * block + index * width, width), width)
            goal = pl.ds(pl.multiple_of(index * width, width), width)
            top, low = split_pair(rows_in[source, :])
            raw_top[goal, :] = top
            raw_low[goal, :] = low
            return carry

        lax.fori_loop(0, block // width, body, 0)
        for slot, there, result in solve_slots(raw_top, raw_low):
            top, low = split_pair(result)
            sol_top[:, there] = top
            sol_low[:, there] = low
            sol_full[:, there] = result
        border_out[spread(part, block), :] = sol_full[:, here_cols]

    reuse_sent = on_diag & (core == sent_part)
    reuse_own = on_diag & (core == own_part)

    def swap(index, thin):
        there = pl.ds(index * width if thin else 0, block - index * width if thin else block)
        return remote(
            sent.at[index, there], got.at[index, there],
            ssend.at[index], srecv.at[index], sibling_id,
        )

    def fill_place(index, later):
        return later * (later - 1) // 2 + index

    def share(index, later):
        return remote(
            got.at[index, pl.ds(later * width, width)], fill.at[fill_place(index, later)],
            tsend.at[index, later], trecv.at[index, later], to_far_id,
        )

    thin_send = core == sent_part
    thin_get = core == own_part

    def by_kind(thin, action):
        @pl.when(thin)
        def _():
            action(True)

        @pl.when(jnp.logical_not(thin))
        def _():
            action(False)

    def arrive(index):
        if index == 0:
            for part in range(chunks):
                swap_first(part).wait_recv()
        else:
            by_kind(thin_get, lambda thin: swap(index, thin).wait_recv())

        @pl.when(thin_get & off_diag)
        def _():
            for later in range(index + 1, chunks):
                share(index, later).start()

    def complete(index):
        for before in range(index):
            goal = pl.ds(before * width, width)

            @pl.when(thin_get & off_diag)
            def _(before=before, goal=goal):
                share(before, index).wait_recv()
                got[index, goal, :] = fill[fill_place(before, index)].T

            @pl.when(thin_get & on_diag)
            def _(before=before, goal=goal):
                got[index, goal, :] = got[before, pl.ds(index * width, width), :].T

    def swap_first(index):
        there = pl.ds(index * width, width)
        return remote(
            sent.at[0, there], got.at[0, there], hsend.at[index], hrecv.at[index], sibling_id
        )

    def make_cols(index):
        there = pl.ds(pl.multiple_of(index * width, width), width)

        @pl.when(off_diag)
        def _():
            where = cols_in.at[there, here_cols]
            for kind, target in ((1, to_side_id), (2, to_over_id), (3, to_over_id), (4, to_over_id)):
                remote(
                    where, where, xsend.at[kind, index], xrecv.at[kind, index], target
                ).wait_recv()

        @pl.when(reuse_own)
        def _():
            cols_in[there, :] = rows_in[group_rows(index), :]

        @pl.when(reuse_sent)
        def _():
            col_top[there, :] = sol_top[there, :]
            col_low[there, :] = sol_low[there, :]

        @pl.when(jnp.logical_not(reuse_sent))
        def _():
            top, low = split_pair(cols_in[there, :])
            for slot, place, result in solve_slots(top, low):
                top_part, low_part = split_pair(result)
                col_top[there, place] = top_part
                col_low[there, place] = low_part
                sol_full[there, place] = result

    def first_step(index, carry):
        there = pl.ds(pl.multiple_of(index * width, width), width)
        source = pl.ds(pl.multiple_of(sent_part * block + index * width, width), width)
        top, low = split_pair(rows_in[source, :])
        for slot, place, result in solve_slots(top, low):
            top_part, low_part = split_pair(result)
            sol_top[there, place] = top_part
            sol_low[there, place] = low_part
            sol_full[there, place] = result
        border_out[source, :] = sol_full[there, here_cols]

        @pl.when(index == 0)
        def _():
            make_cols(0)
            keep_sent(0).wait()

        change = dot_pair(
            (sol_top[there, :], sol_low[there, :]),
            (col_top[pl.ds(0, width), :], col_low[pl.ds(0, width), :]),
        )
        sent[0, there, :] = sent[0, there, :] - change
        for which in range(chunks):
            @pl.when(index == which)
            def _(which=which):
                swap_first(which).start()
        return carry

    lax.fori_loop(0, chunks, first_step, 0)

    @pl.when(on_diag)
    def _():
        for index in range(1, chunks):
            pass_group(index).wait_recv()

            @pl.when(core != sent_part)
            def _(index=index):
                over_last(index).start()

    @pl.when(off_diag)
    def _():
        for index in range(chunks):
            side_group(index).wait_recv()
            pass_group(index).start()

    def send_step(index, carry):
        there = pl.ds(pl.multiple_of(index * width, width), width)
        make_cols(index)
        pltpu.make_async_copy(
            update.at[pl.ds(0, block), pl.ds(0, width)], sent.at[index], osem.at[index]
        ).wait()
        change = dot_pair(
            (sol_top[...], sol_low[...]), (col_top[there, :], col_low[there, :])
        )
        sent[index] = sent[index] - change
        for which in range(1, chunks):
            @pl.when(index == which)
            def _(which=which):
                by_kind(thin_send, lambda thin: swap(which, thin).start())
        return carry

    lax.fori_loop(1, chunks, send_step, 0)

    piece = work[spread(col, piece_cols), spread(row, piece_rows)]
    pivot_out[...] = piece.T

    @pl.when(off_diag)
    def _():
        for index in range(chunks):
            pass_group(index).wait_recv()

    @pl.when(reuse_own)
    def _():
        sol_top[...] = col_top[...]
        sol_low[...] = col_low[...]
        border_out[spread(own_part, block), :] = sol_full[:, here_cols]

    @pl.when(jnp.logical_not(reuse_own))
    def _():
        solve_rows(own_part)

    keep_own.wait()

    def own_step(part, carry):
        there = spread(part, width)
        change = dot_pair(
            (sol_top[...], sol_low[...]), (col_top[there, :], col_low[there, :])
        )
        top, low = split_pair(own[:, there] - change)
        own_top[own_rows, there] = top
        own_low[:, there] = low
        return carry

    lax.fori_loop(0, cols_local // width, own_step, 0)

    keep_map.wait()
    keep_diag.wait()
    row_block = 2 * row + leaf_side
    third = half_rows // 3
    slack = half_rows - block

    def one_hot_rows(which, owner, position, base):
        def body(index, carry):
            here = pl.ds(pl.multiple_of(index * third, third), third)
            goal = maps[pl.ds(owner, 1), spread(position, block)] - base - index * third
            at = lax.broadcasted_iota(jnp.int32, (third, block), 0)
            hot[which, here, :] = jnp.where(at == goal, 1.0, 0.0).astype(jnp.bfloat16)
            return carry

        lax.fori_loop(0, half_rows // third, body, 0)

    def pick_t(left, right):
        return dot_t(left[0], right) + dot_t(left[1], right)

    def pick(left, right):
        return jnp.dot(left, right[0], preferred_element_type=jnp.float32) + jnp.dot(
            left, right[1], preferred_element_type=jnp.float32
        )

    def band(index):
        first = max(0, index * third - slack) // BLOCK * BLOCK
        return pl.ds(first, min(block, -(-(index + 1) * third // BLOCK) * BLOCK) - first)

    one_hot_rows(0, leaf, row_block, row_block * half_rows)
    one_hot_rows(1, leaf, col, col * parent_cols)

    for index in range(3):
        here = pl.ds(index * third, third)
        rows = band(index)
        wide = split_pair(pick(hot[0, here, rows], (own_top[rows, own_cols], own_low[rows, :])))
        raw_top[pl.ds(0, third), pl.ds(0, cols_local)] = wide[0]
        raw_low[pl.ds(0, third), pl.ds(0, cols_local)] = wide[1]
        for part in range(3):
            there = pl.ds(part * third, third)
            cols = band(part)
            result = pick_t(
                (raw_top[pl.ds(0, third), cols], raw_low[pl.ds(0, third), cols]),
                hot[1, there, cols],
            )
            if index == part:
                down = lax.broadcasted_iota(jnp.int32, (third, third), 0)
                across = lax.broadcasted_iota(jnp.int32, (third, third), 1)
                on_line = (down == across) & (row_block == col)
                result = result + jnp.where(on_line, diag_in[0:1, there], 0.0)
            parent_out[here, there] = result

    one_hot_rows(0, flip(leaf), row_block, row_block * half_rows)
    one_hot_rows(1, flip(leaf), col, col * parent_cols)

    for index in range(chunks):
        arrive(index)
        complete(index)
        low = index * width
        there = pl.ds(low, width + slack)
        arrived = split_pair(got[index])
        raw_top[own_rows, pl.ds(0, width)] = arrived[0]
        raw_low[own_rows, pl.ds(0, width)] = arrived[1]

        some = pl.ds(0, width)
        wide = split_pair(
            pick(hot[0], (raw_top[own_rows, some], raw_low[own_rows, some]))
        )
        result = pick_t(wide, hot[1, there, pl.ds(low, width)])
        parent_out[:, there] = parent_out[:, there] + result

    @pl.when(below)
    def _():
        own_below().wait_send()

    @pl.when(off_diag)
    def _():
        for index in range(chunks):
            to_relay(index).wait_send()

    @pl.when(on_diag)
    def _():
        for index in range(chunks):
            from_relay(index).wait_send()
            over_first(index).wait_send()
            over_mate(index).wait_send()
            over_last(index).wait_send()

    border_to(0, 0, to_side_id).wait_send()
    pass_side(0).wait_send()
    for index in range(2):
        border_to(1, index, to_mate_id).wait_send()
    for chunk in range(pieces):
        @pl.when(piece_needed(row, col, chunk))
        def _(chunk=chunk):
            for index in (0, 1, 3):
                own_piece(index, chunk).wait_send()

            @pl.when(on_diag)
            def _():
                own_piece(2, chunk).wait_send()
    for index in range(chunks):
        swap_first(index).wait_send()
        side_group(index).wait_send()
        pass_group(index).wait_send()
    for index in range(1, chunks):
        by_kind(thin_send, lambda thin: swap(index, thin).wait_send())

    @pl.when(thin_get & off_diag)
    def _():
        for index in range(chunks):
            for later in range(index + 1, chunks):
                share(index, later).wait_send()


def store_kernel(*refs):
    copies = [
        pltpu.make_async_copy(refs[index], refs[3 + index], refs[6].at[index])
        for index in range(3)
    ]
    for copy in copies:
        copy.start()
    for copy in copies:
        copy.wait()


def whole_front(pivot, border, update, child_map, parent_diag, order):
    piece_rows, piece_cols = pivot.shape
    rows_local, cols_local = update.shape
    block = rows_local // 2
    width = piece_cols
    chunks = cols_local // width
    pieces = piece_rows // BLOCK
    half_rows = parent_diag.shape[1]
    parent_cols = half_rows
    vmem = pl.BlockSpec(memory_space=pltpu.VMEM)
    anywhere = pl.BlockSpec(memory_space=pl.ANY)
    dma = pltpu.SemaphoreType.DMA
    f32 = jnp.float32
    b16 = jnp.bfloat16
    results = pl.pallas_call(
        front_kernel,
        out_shape=(
            pltpu.VMEM((piece_rows, piece_cols), f32),
            pltpu.VMEM((rows_local, piece_cols), f32),
            pltpu.VMEM((half_rows, parent_cols), f32),
        ),
        in_specs=[pl.BlockSpec(memory_space=pltpu.HBM)] * 5,
        out_specs=(vmem, vmem, vmem),
        scratch_shapes=[
            pltpu.VMEM((order, order), f32),
            pltpu.VMEM((order, order), b16),
            pltpu.VMEM((order, order), b16),
            pltpu.VMEM((BLOCK, BLOCK), f32),
            pltpu.VMEM((BLOCK, BLOCK), f32),
            pltpu.VMEM((BLOCK, BLOCK), f32),
            pltpu.VMEM((3, 2 * BLOCK, order), b16),
            pltpu.VMEM((max(order, block), order), b16),
            pltpu.VMEM((max(order, block), order), b16),
            pltpu.VMEM((max(order, block), order), b16),
            pltpu.VMEM((block, order), b16),
            pltpu.VMEM((block, order), b16),
            pltpu.VMEM((block, order), f32),
            pltpu.VMEM((block, order), b16),
            pltpu.VMEM((block, order), b16),
            pltpu.VMEM((block, cols_local), b16),
            pltpu.VMEM((rows_local, order), f32),
            pltpu.VMEM((block, order), f32),
            pltpu.VMEM((block, piece_cols), f32),
            pltpu.VMEM((chunks, block, width), f32),
            pltpu.VMEM((block, cols_local), f32),
            pltpu.VMEM((chunks, block, width), f32),
            pltpu.VMEM((chunks * (chunks - 1) // 2, width, width), f32),
            pltpu.VMEM(child_map.shape, jnp.int32),
            pltpu.VMEM(parent_diag.shape, f32),
            pltpu.VMEM((2, half_rows, block), b16),
            dma((5,)), dma((4, pieces)), dma((4, pieces)), dma((3, pieces)), dma((3, pieces)),
            dma((3, 2)), dma((3, 2)), dma((5, chunks)), dma((5, chunks)),
            dma((chunks,)), dma((chunks,)), dma((chunks,)),
            dma((chunks, chunks)), dma((chunks, chunks)),
            dma((chunks,)), dma((chunks,)), dma((2, chunks)), dma((2, chunks)),
        ],
        compiler_params=pltpu.CompilerParams(
            vmem_limit_bytes=56 * 2**20, collective_id=0, has_side_effects=True
        ),
        name="whole_front",
    )(pivot, border, update, child_map, parent_diag)
    return pl.pallas_call(
        store_kernel,
        out_shape=tuple(jax.ShapeDtypeStruct(result.shape, f32) for result in results),
        in_specs=[vmem] * 3,
        out_specs=(pl.BlockSpec(memory_space=pltpu.HBM),) * 3,
        scratch_shapes=[dma((3,))],
        compiler_params=pltpu.CompilerParams(vmem_limit_bytes=2**20),
        name="store_results",
    )(*results)


def high_dot_t(left, right):
    return lax.dot_general(
        left, right, (((1,), (1,)), ((), ())), precision=HIGH, preferred_element_type=jnp.float32
    )


def split_two(value):
    top = lax.reduce_precision(value, 8, 7)
    return top.astype(jnp.bfloat16), (value - top).astype(jnp.bfloat16)


def one_hot(targets, size):
    return (jnp.arange(size, dtype=jnp.int32)[:, None] == targets[None, :]).astype(jnp.bfloat16)


def pick_dot(left, right, dims):
    return lax.dot_general(left, right, (dims, ((), ())), preferred_element_type=jnp.float32)


def place_blocks(blocks, rows_to, cols_to, out_rows, out_cols):
    col_hot = one_hot(cols_to, out_cols)
    first = 0
    placed = None
    for block in blocks:
        count = block.shape[0]
        row_hot = one_hot(rows_to[first : first + count], out_rows)
        first += count
        top, rest = split_two(block)
        wide = pick_dot(top, col_hot, ((1,), (1,))) + pick_dot(rest, col_hot, ((1,), (1,)))
        top, rest = split_two(wide)
        part = pick_dot(row_hot, top, ((1,), (0,))) + pick_dot(row_hot, rest, ((1,), (0,)))
        placed = part if placed is None else placed + part
    return placed


def column_border(bord, full_rows, nrow, ncol, cols_local, row_index, col_index):
    rows_local, width = bord.shape
    if nrow == 2 and rows_local % cols_local == 0:
        per_row = rows_local // cols_local
        mine = lax.dynamic_slice_in_dim(full_rows, (col_index % per_row) * cols_local, cols_local, 0)
        received = jnp.zeros((cols_local, full_rows.shape[1]), bord.dtype)
        for shift in range(ncol):
            pairs = []
            for c in range(ncol):
                home = c // per_row
                pairs.append((home * ncol + (c + shift) % ncol, (1 - home) * ncol + c))
            target = (col_index - shift + ncol) % ncol
            part = lax.dynamic_slice_in_dim(bord, (target % per_row) * cols_local, cols_local, 0)
            moved = lax.ppermute(part, ("row", "col"), pairs)
            place = (col_index + shift) % ncol * width
            received = lax.dynamic_update_slice_in_dim(received, moved, place, 1)
        return jnp.where(row_index == col_index // per_row, mine, received)
    whole = lax.all_gather(full_rows, "row", axis=0, tiled=True)
    return lax.dynamic_slice_in_dim(whole, col_index * cols_local, cols_local, 0)


def fits(nrow, ncol, pivot, border, update, child_map, parent_diag):
    rows, cols = update.shape
    half_rows = parent_diag.shape[1]
    return (
        nrow == 2
        and ncol == 4
        and pivot.shape[0] == 2 * pivot.shape[1]
        and rows == 2 * cols
        and border.shape == (rows, pivot.shape[1])
        and child_map.shape[1] == nrow * rows
        and pivot.shape[1] % (2 * BLOCK) == 0
        and cols % pivot.shape[1] == 0
        and half_rows % (3 * BLOCK) == 0
        and half_rows > cols
    )


def on_device(pivot, border, update, child_map, parent_diag):
    nrow = lax.axis_size("row")
    ncol = lax.axis_size("col")
    row_index = lax.axis_index("row")
    col_index = lax.axis_index("col")
    leaf_index = lax.axis_index("leaf")
    piece = pivot[0]
    piece_rows, piece_cols = piece.shape
    if fits(nrow, ncol, piece, border[0], update[0], child_map, parent_diag):
        order = nrow * piece_rows
        outs = whole_front(piece, border[0], update[0], child_map, parent_diag, order)
        return tuple(out[None] for out in outs)
    stacked = lax.all_gather(piece[None], ("row", "col"), axis=0, tiled=True)
    stacked, bord = lax.optimization_barrier((stacked, border[0]))
    upper, inverse = factor(stacked, nrow * piece_rows)
    pivot_out = lax.dynamic_slice(
        upper, (col_index * piece_cols, row_index * piece_rows), (piece_cols, piece_rows)
    ).T

    rows_local = bord.shape[0]
    trailing = update[0]
    cols_local = trailing.shape[1]
    full_rows = lax.all_gather(bord, "col", axis=1, tiled=True)
    col_rows = column_border(bord, full_rows, nrow, ncol, cols_local, row_index, col_index)
    factor_cols = high_dot_t(col_rows, inverse)

    half_rows = parent_diag.shape[1]
    block_rows = 2 * half_rows
    parent_cols = block_rows * nrow // ncol
    side = leaf_index % 2
    partner = leaf_index + 1 - 2 * side
    total_cols = child_map.shape[1]
    own_map = lax.dynamic_slice(child_map, (leaf_index, 0), (1, total_cols))[0]
    partner_map = lax.dynamic_slice(child_map, (partner, 0), (1, total_cols))[0]
    swap = [(source, source ^ 1) for source in range(lax.axis_size("leaf"))]

    map_block = total_cols // max(nrow, ncol)
    halves = rows_local % (2 * map_block) == 0
    if halves:
        kept = rows_local // 2
        own_start = side * kept
        sent_start = (1 - side) * kept

        def schur_rows(start, size):
            rows = lax.dynamic_slice_in_dim(full_rows, start, size, 0)
            below = high_dot_t(rows, inverse)
            part = lax.dynamic_slice_in_dim(trailing, start, size, 0)
            return below, part - high_dot_t(below, factor_cols)

        sent_parts = []
        sibling = []
        chunk = kept // CHUNKS
        for index in range(CHUNKS):
            below, sent = schur_rows(sent_start + index * chunk, chunk)
            sent_parts.append(below)
            sibling.append(lax.ppermute(sent, "leaf", swap))
        sent_below = jnp.concatenate(sent_parts, axis=0)
        own_below, own = schur_rows(own_start, kept)
        own_slice = lax.dynamic_slice_in_dim(own_below, col_index * piece_cols, piece_cols, 1)
        sent_slice = lax.dynamic_slice_in_dim(sent_below, col_index * piece_cols, piece_cols, 1)
        border_out = jnp.where(
            side == 0,
            jnp.concatenate([own_slice, sent_slice], axis=0),
            jnp.concatenate([sent_slice, own_slice], axis=0),
        )
    else:
        kept = rows_local
        own_start = 0
        factor_rows = high_dot_t(full_rows, inverse)
        own = trailing - high_dot_t(factor_rows, factor_cols)
        sibling = [lax.ppermute(own, "leaf", swap)]
        border_out = lax.dynamic_slice_in_dim(factor_rows, col_index * piece_cols, piece_cols, 1)

    def my_half(blocks, mapping):
        rows_to = (
            lax.dynamic_slice_in_dim(mapping, row_index * rows_local + own_start, kept)
            - row_index * block_rows
            - side * half_rows
        )
        cols_to = (
            lax.dynamic_slice_in_dim(mapping, col_index * cols_local, cols_local)
            - col_index * parent_cols
        )
        return place_blocks(blocks, rows_to, cols_to, half_rows, parent_cols)

    global_rows = row_index * block_rows + side * half_rows + jnp.arange(half_rows, dtype=jnp.int32)
    global_cols = col_index * parent_cols + jnp.arange(parent_cols, dtype=jnp.int32)
    diagonal = jnp.where(global_rows[:, None] == global_cols[None, :], parent_diag[0][:, None], 0.0)
    parent_out = my_half([own], own_map) + diagonal + my_half(sibling, partner_map)
    return (pivot_out[None], border_out[None], parent_out[None])


def solution(mesh):
    placed = (
        P("leaf", "row", "col"),
        P("leaf", "row", "col"),
        P("leaf", "row", "col"),
        P(),
        P("leaf", "row"),
    )
    return jax.shard_map(
        on_device,
        mesh=mesh,
        in_specs=placed,
        out_specs=(P("leaf", "row", "col"), P("leaf", "row", "col"), P("leaf", "row", "col")),
        check_vma=False,
    )
```
